64 devices in a mesh: dp: 4 (over x, y), tp: 16 (over z, core).
Axes of the slice: x: 2, y: 2, z: 8, core: 2. Of those that a mesh axis runs over, the one named last changes fastest.
The devices are a block of a 4x4x8 slice.
Arguments:
- hidden: bfloat16 [32, 16, 3072], P('dp'), parts along dimension 0
- norm_w: bfloat16 [3072], replicated
- embedding: bfloat16 [256000, 3072], P('tp')
- draft_ids: int32 [32, 16], P('dp'), parts along dimension 0
Outputs:
- output 1: float32 [32, 16], P('dp'), parts along dimension 0
- output 2: float32 [32, 16], P('dp'), parts along dimension 0
There are 4 independent parts. The reference program is written for one: setup_inputs(seed, part) draws one part's arguments, and reference() takes and returns one part's arrays. A program takes and returns all parts, laid end to end along the dimension named above; an argument that names none is the same for every part.
All inputs are finite; a program needn't handle non-finite values.
Results may differ from the reference program's by a relative error of at most 0.001.
Values sent between devices are 32-bit elements.
A program may use at most 768 MiB of HBM per device.

```python
import jax
import jax.numpy as jnp
from jax import lax

BATCH = 8
DRAFT = 16
D = 3072
VOCAB = 256000
EPS = 1e-6
ROW_BLOCK = 2 ** 11
HOT_IDS = VOCAB // 16
ALIGN_SCALE = 6.0
NOISE_SCALE = 3.0


def draw_embedding(key_coef, key_noise, direction):
    num_blocks = VOCAB // ROW_BLOCK

    def one_block(block_idx):
        tok_coef = jax.random.normal(jax.random.fold_in(key_coef, block_idx), (ROW_BLOCK, 1), jnp.float32)
        noise_rows = jax.random.normal(jax.random.fold_in(key_noise, block_idx), (ROW_BLOCK, D), jnp.float32)
        block_rows = ALIGN_SCALE * tok_coef * direction / D + NOISE_SCALE * noise_rows * D ** -0.5
        return block_rows.astype(jnp.bfloat16)

    return lax.map(one_block, jnp.arange(num_blocks)).reshape(VOCAB, D)


def setup_inputs(seed: int = 0, part: int = 0) -> dict:
    base_key = jax.random.key(seed)
    key_dir, key_w, key_coef, key_noise, key_part = jax.random.split(base_key, 5)
    key_part = jax.random.fold_in(key_part, part)
    key_mix, key_hid, key_pick, key_low, key_any = jax.random.split(key_part, 5)
    direction = jax.random.normal(key_dir, (D,), jnp.float32)
    mix_coef = jax.random.uniform(key_mix, (BATCH, DRAFT, 1), jnp.float32, -0.9, 0.9)
    hid_noise = jax.random.normal(key_hid, (BATCH, DRAFT, D), jnp.float32)
    hidden = mix_coef * direction + jnp.sqrt(1.0 - mix_coef * mix_coef) * hid_noise
    norm_w = 0.5 * jax.random.normal(key_w, (D,), jnp.float32)
    embedding = draw_embedding(key_coef, key_noise, direction)
    pick_kind = jax.random.randint(key_pick, (BATCH, DRAFT), 0, 4)
    low_ids = jax.random.randint(key_low, (BATCH, DRAFT), 0, HOT_IDS)
    any_ids = jax.random.randint(key_any, (BATCH, DRAFT), 0, VOCAB)
    draft_ids = jnp.where(pick_kind < 3, low_ids, any_ids).astype(jnp.int32)
    draft_ids = draft_ids.at[0, 0].set(VOCAB - 1).at[0, 1].set(0)
    return {"hidden": hidden.astype(jnp.bfloat16), "norm_w": norm_w.astype(jnp.bfloat16), "embedding": embedding, "draft_ids": draft_ids}


def reference(hidden, norm_w, embedding, draft_ids):
    gain = 1.0 + norm_w.astype(jnp.float32)

    def one_seq(seq_args):
        seq_hidden, seq_ids = seq_args
        x_float = seq_hidden.astype(jnp.float32)
        mean_sq = jnp.mean(x_float * x_float, axis=-1, keepdims=True)
        normed = (x_float * lax.rsqrt(mean_sq + EPS) * gain).astype(jnp.bfloat16)
        logits = jnp.dot(normed, embedding.T, preferred_element_type=jnp.float32)
        row_max = jnp.max(logits, axis=-1, keepdims=True)
        exp_shift = jnp.exp(logits - row_max)
        exp_total = jnp.sum(exp_shift, axis=-1)
        weighted = jnp.sum(exp_shift * logits, axis=-1)
        log_norm = row_max[:, 0] + jnp.log(exp_total)
        picked = jnp.take_along_axis(logits, seq_ids[:, None], axis=-1)[:, 0]
        return picked - log_norm, log_norm - weighted / exp_total

    log_prob, entropy = lax.map(one_seq, (hidden, draft_ids))
    return log_prob, entropy
```

```python
import functools

import jax
import jax.numpy as jnp
from jax import lax
from jax.experimental import pallas as pl
from jax.experimental.pallas import tpu as pltpu
from jax.sharding import PartitionSpec as P

EPS = 1e-6
MESH = pl.DeviceIdType.MESH
ROWS = 800
SLOTS = 8
HALF = ROWS // 2
LANES = 128
SUB = 8


def _peer(rank):
    return {"tp": rank}


def _stats_update(z, first_row, ids, stats):
    top, total, weighted, picked = stats
    rows, width = z.shape
    cube = z.reshape(rows // SUB, SUB, width)
    new_top = jnp.maximum(top, jnp.max(cube, axis=0))
    scale = jnp.exp(top - new_top)
    probs = jnp.exp(cube - new_top[None])
    total = total * scale + jnp.sum(probs, axis=0)
    weighted = weighted * scale + jnp.sum(probs * cube, axis=0)
    row_ids = lax.broadcasted_iota(jnp.int32, (rows, width), 0) + first_row
    hit = jnp.where(row_ids == ids, z, 0.0)
    picked = picked + jnp.sum(hit.reshape(rows // SUB, SUB, width), axis=0)
    return new_top, total, weighted, picked


def _kernel(tp, shard_rows, hidden_hbm, gain_ref, ids_ref, emb_hbm, out_ref, hid, wts, ring, even, odd, mine, board, hid_sem, ring_sem, send_sem, recv_sem):
    me = lax.axis_index("tp")
    chunks = shard_rows // ROWS
    depth = wts.shape[0]

    hid_copy = pltpu.make_async_copy(hidden_hbm, hid, hid_sem)
    hid_copy.start()

    def chunk_copy(idx, slot):
        return pltpu.make_async_copy(emb_hbm.at[pl.ds(pl.multiple_of(idx * ROWS, ROWS), ROWS)], ring.at[slot], ring_sem.at[slot])

    for idx in range(min(SLOTS, chunks)):
        chunk_copy(idx, idx).start()

    barrier = pltpu.get_barrier_semaphore()
    for step in range(1, tp):
        pl.semaphore_signal(barrier, inc=1, device_id=_peer(lax.rem(me + step, tp)), device_id_type=MESH)

    hid_copy.wait()
    gain = 1.0 + gain_ref[...].astype(jnp.float32)
    x = hid[...].astype(jnp.float32)
    mean_sq = jnp.sum(x * x, axis=-1, keepdims=True) / depth
    normed = x * lax.rsqrt(mean_sq + EPS) * gain
    wts[...] = normed.T.astype(jnp.bfloat16)

    ids = ids_ref[...] - me * shard_rows

    low = jnp.full((SUB, LANES), jnp.finfo(jnp.float32).min, jnp.float32)
    zero = jnp.zeros((SUB, LANES), jnp.float32)

    def multiply(idx, dst):
        slot = lax.rem(idx, SLOTS)
        chunk_copy(idx, slot).wait()
        stationary = wts[...]
        for part in range(2):
            rows = slice(part * HALF, (part + 1) * HALF)
            dst[rows] = jnp.dot(ring[slot, rows], stationary, preferred_element_type=jnp.float32)

    def refill(idx):
        @pl.when(idx + SLOTS < chunks)
        def _():
            chunk_copy(idx + SLOTS, lax.rem(idx, SLOTS)).start()

    def reduce(idx, src, stats):
        return _stats_update(src[...], idx * ROWS, ids, stats)

    multiply(0, even)
    refill(0)

    def body(pair, stats):
        idx = 2 * pair
        multiply(idx + 1, odd)
        stats = reduce(idx, even, stats)
        refill(idx + 1)
        multiply(idx + 2, even)
        stats = reduce(idx + 1, odd, stats)
        refill(idx + 2)
        return stats

    stats = lax.fori_loop(0, (chunks - 1) // 2, body, (low, zero, zero, zero))
    last = even
    if chunks % 2 == 0:
        multiply(chunks - 1, odd)
        stats = reduce(chunks - 2, even, stats)
        last = odd
    stats = reduce(chunks - 1, last, stats)

    top, total, weighted, picked = stats
    best = jnp.max(top, axis=0, keepdims=True)
    scale = jnp.exp(top - best)
    mine[0:1] = best
    mine[1:2] = jnp.sum(total * scale, axis=0, keepdims=True)
    mine[2:3] = jnp.sum(weighted * scale, axis=0, keepdims=True)
    mine[3:4] = jnp.sum(picked, axis=0, keepdims=True)
    mine[4:8] = jnp.zeros((4, LANES), jnp.float32)

    pl.semaphore_wait(barrier, tp - 1)

    def send(step):
        return pltpu.make_async_remote_copy(
            src_ref=mine, dst_ref=board.at[me], send_sem=send_sem.at[step], recv_sem=recv_sem.at[me],
            device_id=_peer(lax.rem(me + step, tp)), device_id_type=MESH)

    def receive(step):
        rank = lax.rem(me + step, tp)
        return pltpu.make_async_remote_copy(
            src_ref=mine, dst_ref=board.at[rank], send_sem=send_sem.at[step], recv_sem=recv_sem.at[rank],
            device_id=_peer(rank), device_id_type=MESH)

    for step in range(1, tp):
        send(step).start()
    board[me] = mine[...]
    for step in range(1, tp):
        receive(step).wait_recv()
    for step in range(1, tp):
        send(step).wait_send()

    every = board[...]
    tops = every[:, 0]
    row_max = jnp.max(tops, axis=0, keepdims=True)
    scale = jnp.exp(tops - row_max)
    exp_total = jnp.sum(every[:, 1] * scale, axis=0, keepdims=True)
    weighted = jnp.sum(every[:, 2] * scale, axis=0, keepdims=True)
    picked = jnp.sum(every[:, 3], axis=0, keepdims=True)
    log_norm = row_max + jnp.log(exp_total)
    out_ref[0:1] = picked - log_norm
    out_ref[1:2] = log_norm - weighted / exp_total


def solution(mesh):
    tp = mesh.shape["tp"]

    def local_part(hidden, norm_w, embedding, draft_ids):
        seqs, drafts, depth = hidden.shape
        positions = seqs * drafts
        shard_rows = embedding.shape[0]
        vmem = pl.BlockSpec(memory_space=pltpu.VMEM)
        hbm = pl.BlockSpec(memory_space=pl.ANY)
        out = pl.pallas_call(
            functools.partial(_kernel, tp, shard_rows),
            out_shape=jax.ShapeDtypeStruct((2, positions), jnp.float32),
            in_specs=[hbm, vmem, vmem, hbm],
            out_specs=vmem,
            scratch_shapes=[
                pltpu.VMEM((positions, depth), jnp.bfloat16),
                pltpu.VMEM((depth, positions), jnp.bfloat16),
                pltpu.VMEM((SLOTS, ROWS, depth), jnp.bfloat16),
                pltpu.VMEM((ROWS, positions), jnp.float32),
                pltpu.VMEM((ROWS, positions), jnp.float32),
                pltpu.VMEM((SUB, positions), jnp.float32),
                pltpu.VMEM((tp, SUB, positions), jnp.float32),
                pltpu.SemaphoreType.DMA,
                pltpu.SemaphoreType.DMA((SLOTS,)),
                pltpu.SemaphoreType.DMA((tp,)),
                pltpu.SemaphoreType.DMA((tp,)),
            ],
            compiler_params=pltpu.CompilerParams(collective_id=0, has_side_effects=True, vmem_limit_bytes=62 * 2**20),
            name="vocab_head",
        )(hidden.reshape(positions, depth), norm_w.reshape(1, depth), draft_ids.reshape(1, positions), embedding)
        return out[0].reshape(seqs, drafts), out[1].reshape(seqs, drafts)

    return jax.shard_map(local_part, mesh=mesh, in_specs=(P("dp", None, None), P(None), P("tp", None), P("dp", None)), out_specs=(P("dp", None), P("dp", None)), check_vma=False)
```

```python
import functools

import jax
import jax.numpy as jnp
from jax import lax
from jax.experimental import pallas as pl
from jax.experimental.pallas import tpu as pltpu
from jax.sharding import PartitionSpec as P

EPS = 1e-6
MESH = pl.DeviceIdType.MESH
ROWS = 800
SLOTS = 8
HALF = ROWS // 2
LANES = 128
SUB = 8


def _peer(rank):
    return {"tp": rank}


def _stats_update(z, first_row, ids, stats):
    top, total, weighted, picked = stats
    rows, width = z.shape
    cube = z.reshape(rows // SUB, SUB, width)
    new_top = jnp.maximum(top, jnp.max(cube, axis=0))
    scale = jnp.exp(top - new_top)
    probs = jnp.exp(cube - new_top[None])
    total = total * scale + jnp.sum(probs, axis=0)
    weighted = weighted * scale + jnp.sum(probs * cube, axis=0)
    row_ids = lax.broadcasted_iota(jnp.int32, (rows, width), 0) + first_row
    hit = jnp.where(row_ids == ids, z, 0.0)
    picked = picked + jnp.sum(hit.reshape(rows // SUB, SUB, width), axis=0)
    return new_top, total, weighted, picked


def _kernel(tp, hidden_hbm, gain_hbm, ids_hbm, emb_hbm, lp_ref, ent_ref, hid, gain_vm, ids_vm, wts, ring, even, odd, mine, board, hid_sem, gain_sem, ids_sem, ring_sem, send_sem, recv_sem):
    me = lax.axis_index("tp")
    shard_rows, depth = emb_hbm.shape
    chunks = shard_rows // ROWS
    seqs, drafts = lp_ref.shape

    hid_copy = pltpu.make_async_copy(hidden_hbm, hid, hid_sem)
    gain_copy = pltpu.make_async_copy(gain_hbm, gain_vm, gain_sem)
    ids_copy = pltpu.make_async_copy(ids_hbm, ids_vm, ids_sem)
    hid_copy.start(priority=0)
    gain_copy.start(priority=0)
    ids_copy.start(priority=0)

    def chunk_copy(idx, slot):
        return pltpu.make_async_copy(emb_hbm.at[pl.ds(pl.multiple_of(idx * ROWS, ROWS), ROWS)], ring.at[slot], ring_sem.at[slot])

    for idx in range(min(SLOTS, chunks)):
        chunk_copy(idx, idx).start(priority=1)

    barrier = pltpu.get_barrier_semaphore()
    for step in range(1, tp):
        pl.semaphore_signal(barrier, inc=1, device_id=_peer(lax.rem(me + step, tp)), device_id_type=MESH)

    gain_copy.wait()
    ids_copy.wait()
    hid_copy.wait()
    gain = 1.0 + gain_vm[...].astype(jnp.float32)[None]
    x = hid[...].astype(jnp.float32)
    mean_sq = jnp.sum(x * x, axis=-1, keepdims=True) / depth
    normed = x * lax.rsqrt(mean_sq + EPS) * gain
    wts[...] = normed.T.astype(jnp.bfloat16)

    grid_ids = ids_vm[...] - me * shard_rows
    ids = jnp.concatenate([grid_ids[seq:seq + 1] for seq in range(seqs)], axis=1)

    low = jnp.full((SUB, LANES), jnp.finfo(jnp.float32).min, jnp.float32)
    zero = jnp.zeros((SUB, LANES), jnp.float32)

    def multiply(idx, dst):
        slot = lax.rem(idx, SLOTS)
        chunk_copy(idx, slot).wait()
        stationary = wts[...]
        for part in range(2):
            rows = slice(part * HALF, (part + 1) * HALF)
            dst[rows] = jnp.dot(ring[slot, rows], stationary, preferred_element_type=jnp.float32)

    def refill(idx):
        @pl.when(idx + SLOTS < chunks)
        def _():
            chunk_copy(idx + SLOTS, lax.rem(idx, SLOTS)).start(priority=1)

    def reduce(idx, src, stats):
        return _stats_update(src[...], idx * ROWS, ids, stats)

    multiply(0, even)
    refill(0)

    def body(pair, stats):
        idx = 2 * pair
        multiply(idx + 1, odd)
        stats = reduce(idx, even, stats)
        refill(idx + 1)
        multiply(idx + 2, even)
        stats = reduce(idx + 1, odd, stats)
        refill(idx + 2)
        return stats

    stats = lax.fori_loop(0, (chunks - 1) // 2, body, (low, zero, zero, zero))
    last = even
    if chunks % 2 == 0:
        multiply(chunks - 1, odd)
        stats = reduce(chunks - 2, even, stats)
        last = odd
    stats = reduce(chunks - 1, last, stats)

    top, total, weighted, picked = stats
    best = jnp.max(top, axis=0, keepdims=True)
    scale = jnp.exp(top - best)
    mine[0:1] = best
    mine[1:2] = jnp.sum(total * scale, axis=0, keepdims=True)
    mine[2:3] = jnp.sum(weighted * scale, axis=0, keepdims=True)
    mine[3:4] = jnp.sum(picked, axis=0, keepdims=True)
    mine[4:8] = jnp.zeros((4, LANES), jnp.float32)

    pl.semaphore_wait(barrier, tp - 1)

    def send(step):
        return pltpu.make_async_remote_copy(
            src_ref=mine, dst_ref=board.at[me], send_sem=send_sem.at[step], recv_sem=recv_sem.at[me],
            device_id=_peer(lax.rem(me + step, tp)), device_id_type=MESH)

    def receive(step):
        rank = lax.rem(me + step, tp)
        return pltpu.make_async_remote_copy(
            src_ref=mine, dst_ref=board.at[rank], send_sem=send_sem.at[step], recv_sem=recv_sem.at[rank],
            device_id=_peer(rank), device_id_type=MESH)

    for step in range(1, tp):
        send(step).start()
    board[me] = mine[...]
    for step in range(1, tp):
        receive(step).wait_recv()
    for step in range(1, tp):
        send(step).wait_send()

    every = board[...]
    tops = every[:, 0]
    row_max = jnp.max(tops, axis=0, keepdims=True)
    scale = jnp.exp(tops - row_max)
    exp_total = jnp.sum(every[:, 1] * scale, axis=0, keepdims=True)
    weighted = jnp.sum(every[:, 2] * scale, axis=0, keepdims=True)
    picked = jnp.sum(every[:, 3], axis=0, keepdims=True)
    log_norm = row_max + jnp.log(exp_total)
    log_prob = picked - log_norm
    entropy = log_norm - weighted / exp_total
    for seq in range(seqs):
        lanes = slice(seq * drafts, (seq + 1) * drafts)
        lp_ref[seq:seq + 1] = log_prob[:, lanes]
        ent_ref[seq:seq + 1] = entropy[:, lanes]


def solution(mesh):
    tp = mesh.shape["tp"]

    def local_part(hidden, norm_w, embedding, draft_ids):
        seqs, drafts, depth = hidden.shape
        positions = seqs * drafts
        vmem = pl.BlockSpec(memory_space=pltpu.VMEM)
        hbm = pl.BlockSpec(memory_space=pl.ANY)
        grid = jax.ShapeDtypeStruct((seqs, drafts), jnp.float32)
        return pl.pallas_call(
            functools.partial(_kernel, tp),
            out_shape=(grid, grid),
            in_specs=[hbm] * 4,
            out_specs=(vmem, vmem),
            scratch_shapes=[
                pltpu.VMEM((positions, depth), jnp.bfloat16),
                pltpu.VMEM((depth,), jnp.bfloat16),
                pltpu.VMEM((seqs, drafts), jnp.int32),
                pltpu.VMEM((depth, positions), jnp.bfloat16),
                pltpu.VMEM((SLOTS, ROWS, depth), jnp.bfloat16),
                pltpu.VMEM((ROWS, positions), jnp.float32),
                pltpu.VMEM((ROWS, positions), jnp.float32),
                pltpu.VMEM((SUB, positions), jnp.float32),
                pltpu.VMEM((tp, SUB, positions), jnp.float32),
                pltpu.SemaphoreType.DMA,
                pltpu.SemaphoreType.DMA,
                pltpu.SemaphoreType.DMA,
                pltpu.SemaphoreType.DMA((SLOTS,)),
                pltpu.SemaphoreType.DMA((tp,)),
                pltpu.SemaphoreType.DMA((tp,)),
            ],
            compiler_params=pltpu.CompilerParams(collective_id=0, has_side_effects=True, vmem_limit_bytes=62 * 2**20),
            name="vocab_head",
        )(hidden.reshape(positions, depth), norm_w, draft_ids, embedding)

    return jax.shard_map(local_part, mesh=mesh, in_specs=(P("dp", None, None), P(None), P("tp", None), P("dp", None)), out_specs=(P("dp", None), P("dp", None)), check_vma=False)
```

```python
import functools

import jax
import jax.numpy as jnp
from jax import lax
from jax.experimental import pallas as pl
from jax.experimental.pallas import tpu as pltpu
from jax.sharding import PartitionSpec as P

EPS = 1e-6
MESH = pl.DeviceIdType.MESH
ROWS = 800
HALF = ROWS // 2
SLOTS = 8
SOLO = 8
LANES = 128
SUB = 8
STATS = 4
QUARTERS = 4


def _stats_update(z, first_row, ids, stats):
    top, total, weighted, picked = stats
    rows, width = z.shape
    cube = z.reshape(rows // SUB, SUB, width)
    new_top = jnp.maximum(top, jnp.max(cube, axis=0))
    scale = jnp.exp(top - new_top)
    probs = jnp.exp(cube - new_top[None])
    total = total * scale + jnp.sum(probs, axis=0)
    weighted = weighted * scale + jnp.sum(probs * cube, axis=0)
    row_ids = lax.broadcasted_iota(jnp.int32, (rows, width), 0) + first_row
    hit = jnp.where(row_ids == ids, z, 0.0)
    picked = picked + jnp.sum(hit.reshape(rows // SUB, SUB, width), axis=0)
    return new_top, total, weighted, picked


def _kernel(tp, hidden_hbm, gain_hbm, ids_hbm, emb_hbm, out_ref, hid, gain_vm, ids_vm, wts, outbox, inbox, ring, logits, mine, board,
            hid_sem, gain_sem, ids_sem, ids_sems, ring_sem, hop_send, hop_recv, send_sem, recv_sem):
    me = lax.axis_index("tp")
    group = lax.axis_index("dp")
    parity = lax.rem(group, 2)
    other = group + 1 - 2 * parity
    core = lax.rem(me, 2)
    chip = me // 2
    chips = tp // 2
    shard_rows, depth = emb_hbm.shape
    columns = depth // 2
    pair_chunks = (shard_rows // ROWS - SOLO) // 2
    chunks = SOLO + pair_chunks
    _, seqs, drafts = out_ref.shape
    positions = seqs * drafts
    quarter = positions // QUARTERS
    tiles = quarter // SUB

    hid_copy = pltpu.make_async_copy(hidden_hbm, hid, hid_sem)
    gain_copy = pltpu.make_async_copy(gain_hbm, gain_vm, gain_sem)
    ids_copy = pltpu.make_async_copy(ids_hbm, ids_vm.at[0], ids_sem)
    hid_copy.start(priority=0)
    gain_copy.start(priority=0)
    ids_copy.start(priority=0)

    def first_row(idx):
        return (idx + jnp.where(idx < SOLO, 0, parity * pair_chunks)) * ROWS

    def chunk_copy(idx):
        slot = lax.rem(idx, SLOTS)
        return pltpu.make_async_copy(emb_hbm.at[pl.ds(pl.multiple_of(first_row(idx), ROWS), ROWS)], ring.at[slot], ring_sem.at[slot])

    for idx in range(min(SLOTS, chunks)):
        chunk_copy(idx).start(priority=1)

    own_steps = sorted(range(1, tp), key=lambda step: -min(step, tp - step))
    all_steps = sorted(range(tp), key=lambda step: -min(step, tp - step))
    barrier = pltpu.get_barrier_semaphore()
    for step in own_steps:
        pl.semaphore_signal(barrier, inc=1, device_id={"dp": group, "tp": lax.rem(me + step, tp)}, device_id_type=MESH)
    for step in all_steps:
        pl.semaphore_signal(barrier, inc=1, device_id={"dp": other, "tp": lax.rem(me + step, tp)}, device_id_type=MESH)

    gain_copy.wait()
    hid_copy.wait()
    gain = 1.0 + gain_vm[...].astype(jnp.float32)[None]

    def normalize(x):
        x = x.astype(jnp.float32)
        mean_sq = jnp.sum(x * x, axis=-1, keepdims=True) / depth
        return (x * lax.rsqrt(mean_sq + EPS) * gain).astype(jnp.bfloat16)

    def quarter_of(turn):
        return lax.rem(chip + turn, QUARTERS)

    for turn in (0, 2):
        start = pl.multiple_of(quarter_of(turn) * quarter, quarter)
        outbox[turn // 2] = normalize(hid[pl.ds(start, quarter)]).astype(jnp.float32)

    def spot(turn, tile, side):
        return inbox.at[quarter_of(turn), pl.ds(tile * SUB, SUB), pl.ds(pl.multiple_of(side * columns, columns), columns)]

    def arrival(turn, tile, side):
        return hop_recv.at[(quarter_of(turn) * tiles + tile) * 2 + side]

    def hop(src, turn, tile, side, slot, device):
        return pltpu.make_async_remote_copy(
            src_ref=src, dst_ref=spot(turn, tile, side), send_sem=hop_send.at[slot], recv_sem=arrival(turn, tile, side),
            device_id=device, device_id_type=MESH)

    def across(turn, tile):
        src = outbox.at[turn // 2, pl.ds(tile * SUB, SUB), pl.ds(pl.multiple_of(core * columns, columns), columns)]
        return hop(src, turn, tile, core, (turn // 2) * tiles + tile, {"dp": other, "tp": me})

    def along(tile, up):
        next_chip = lax.rem(chip + (1 if up else chips - 1), chips)
        return hop(spot(0, tile, core), 0, tile, core, (2 if up else 3) * tiles + tile, {"dp": group, "tp": 2 * next_chip + core})

    def sideways(turn, tile):
        return hop(spot(turn, tile, core), turn, tile, core, (4 + turn) * tiles + tile, {"dp": group, "tp": me + 1 - 2 * core})

    def landed(turn, tile, side):
        hop(spot(turn, tile, side), turn, tile, side, 0, {"dp": group, "tp": me}).wait_recv()

    ids_copy.wait()
    pl.semaphore_wait(barrier, 2 * tp - 1)
    for turn in (0, 2):
        for tile in range(tiles):
            across(turn, tile).start()
    ids_hop = pltpu.make_async_remote_copy(
        src_ref=ids_vm.at[0], dst_ref=ids_vm.at[1], send_sem=ids_sems.at[0], recv_sem=ids_sems.at[1],
        device_id={"dp": other, "tp": me}, device_id_type=MESH)
    ids_hop.start()

    wts[:positions] = normalize(hid[...])

    def pass_on(tile):
        landed(0, tile, core)
        along(tile, True).start()
        along(tile, False).start()

    def swap(turn, tile):
        if turn:
            landed(turn, tile, core)
        sideways(turn, tile).start()

    agenda = {
        2: [(pass_on, 0)],
        3: [(pass_on, 1)],
        4: [(pass_on, 2), (pass_on, 3)],
        5: [(swap, 0, tile) for tile in range(tiles)],
        6: [(swap, 2, 0), (swap, 2, 1), (swap, 1, 0), (swap, 3, 0)],
        7: [(swap, 1, 1), (swap, 3, 1), (swap, 1, 2), (swap, 3, 2), (swap, 1, 3), (swap, 3, 3), (swap, 2, 2), (swap, 2, 3)],
    }

    def row_ids(which):
        table = ids_vm[which] - me * shard_rows
        return jnp.concatenate([table[seq:seq + 1] for seq in range(seqs)], axis=1)

    own_ids = row_ids(0)
    low = jnp.full((SUB, positions), jnp.finfo(jnp.float32).min, jnp.float32)
    zero = jnp.zeros((SUB, positions), jnp.float32)

    def multiply(idx, width):
        slot = lax.rem(idx, SLOTS)
        stationary = wts[:width]
        for part in range(2):
            rows = slice(part * HALF, (part + 1) * HALF)
            logits[rows, :width] = lax.dot_general(ring[slot, rows], stationary, (((1,), (1,)), ((), ())), preferred_element_type=jnp.float32)

    def refill(idx):
        @pl.when(idx + SLOTS < chunks)
        def _():
            chunk_copy(idx + SLOTS).start(priority=1)

    def reduce(idx, width, ids, stats):
        return _stats_update(logits[:, :width], first_row(idx), ids, stats)

    chunk_copy(0).wait()
    multiply(0, positions)
    refill(0)

    def solo(idx, stats):
        for when, deeds in agenda.items():
            @pl.when(idx == when)
            def _(deeds=deeds):
                for deed, *what in deeds:
                    deed(*what)
        chunk_copy(idx).wait()
        stats = reduce(idx - 1, positions, own_ids, stats)
        multiply(idx, positions)
        refill(idx)
        return stats

    stats = lax.fori_loop(1, SOLO, solo, (low, zero, zero, zero))

    for turn in range(QUARTERS):
        for tile in range(tiles):
            landed(turn, tile, 1 - core)
    ids_hop.wait_recv()
    wts[positions:] = inbox[...].reshape(positions, depth).astype(jnp.bfloat16)
    both_ids = jnp.concatenate([own_ids, row_ids(1)], axis=1)

    chunk_copy(SOLO).wait()
    stats = reduce(SOLO - 1, positions, own_ids, stats)
    multiply(SOLO, 2 * positions)
    refill(SOLO)
    stats = tuple(jnp.concatenate([mine_part, start], axis=1) for mine_part, start in zip(stats, (low, zero, zero, zero)))

    def paired(idx, stats):
        chunk_copy(idx).wait()
        stats = reduce(idx - 1, 2 * positions, both_ids, stats)
        multiply(idx, 2 * positions)
        refill(idx)
        return stats

    stats = lax.fori_loop(SOLO + 1, chunks, paired, stats)
    top, total, weighted, picked = reduce(chunks - 1, 2 * positions, both_ids, stats)

    best = jnp.max(top, axis=0, keepdims=True)
    scale = jnp.exp(top - best)
    summary = (
        best,
        jnp.sum(total * scale, axis=0, keepdims=True),
        jnp.sum(weighted * scale, axis=0, keepdims=True),
        jnp.sum(picked, axis=0, keepdims=True),
    )
    for side in range(2):
        for row, value in enumerate(summary):
            mine[side, row:row + 1] = value[:, side * positions:(side + 1) * positions]

    def report(side, step):
        return pltpu.make_async_remote_copy(
            src_ref=mine.at[side], dst_ref=board.at[side * tp + me], send_sem=send_sem.at[side * tp + step], recv_sem=recv_sem.at[side * tp + me],
            device_id={"dp": other if side else group, "tp": lax.rem(me + step, tp)}, device_id_type=MESH)

    def reported(side, step):
        rank = lax.rem(me + step, tp)
        return pltpu.make_async_remote_copy(
            src_ref=mine.at[side], dst_ref=board.at[side * tp + rank], send_sem=send_sem.at[side * tp + step], recv_sem=recv_sem.at[side * tp + rank],
            device_id={"dp": other if side else group, "tp": rank}, device_id_type=MESH)

    for step in all_steps:
        report(1, step).start()
        if step:
            report(0, step).start()
    board[me] = mine[0]

    ids_hop.wait_send()
    for turn in (0, 2):
        for tile in range(tiles):
            across(turn, tile).wait_send()
    for tile in range(tiles):
        along(tile, True).wait_send()
        along(tile, False).wait_send()
    for turn in range(QUARTERS):
        for tile in range(tiles):
            sideways(turn, tile).wait_send()

    for step in all_steps:
        reported(1, step).wait_recv()
        if step:
            reported(0, step).wait_recv()
    for step in all_steps:
        report(1, step).wait_send()
        if step:
            report(0, step).wait_send()

    every = board[...]
    tops = every[:, 0]
    row_max = jnp.max(tops, axis=0, keepdims=True)
    scale = jnp.exp(tops - row_max)
    exp_total = jnp.sum(every[:, 1] * scale, axis=0, keepdims=True)
    weighted = jnp.sum(every[:, 2] * scale, axis=0, keepdims=True)
    picked = jnp.sum(every[:, 3], axis=0, keepdims=True)
    log_norm = row_max + jnp.log(exp_total)
    log_prob = picked - log_norm
    entropy = log_norm - weighted / exp_total
    for seq in range(seqs):
        lanes = slice(seq * drafts, (seq + 1) * drafts)
        out_ref[0, seq:seq + 1] = log_prob[:, lanes]
        out_ref[1, seq:seq + 1] = entropy[:, lanes]


def solution(mesh):
    tp = mesh.shape["tp"]

    def local_part(hidden, norm_w, embedding, draft_ids):
        seqs, drafts, depth = hidden.shape
        positions = seqs * drafts
        tiles = positions // QUARTERS // SUB
        hbm = pl.BlockSpec(memory_space=pl.ANY)
        out = pl.pallas_call(
            functools.partial(_kernel, tp),
            out_shape=jax.ShapeDtypeStruct((2, seqs, drafts), jnp.float32),
            in_specs=[hbm] * 4,
            out_specs=pl.BlockSpec(memory_space=pltpu.VMEM),
            scratch_shapes=[
                pltpu.VMEM((positions, depth), jnp.bfloat16),
                pltpu.VMEM((depth,), jnp.bfloat16),
                pltpu.VMEM((2, seqs, drafts), jnp.int32),
                pltpu.VMEM((2 * positions, depth), jnp.bfloat16),
                pltpu.VMEM((2, positions // QUARTERS, depth), jnp.float32),
                pltpu.VMEM((QUARTERS, positions // QUARTERS, depth), jnp.float32),
                pltpu.VMEM((SLOTS, ROWS, depth), jnp.bfloat16),
                pltpu.VMEM((ROWS, 2 * positions), jnp.float32),
                pltpu.VMEM((2, STATS, positions), jnp.float32),
                pltpu.VMEM((2 * tp, STATS, positions), jnp.float32),
                pltpu.SemaphoreType.DMA,
                pltpu.SemaphoreType.DMA,
                pltpu.SemaphoreType.DMA,
                pltpu.SemaphoreType.DMA((2,)),
                pltpu.SemaphoreType.DMA((SLOTS,)),
                pltpu.SemaphoreType.DMA((8 * tiles,)),
                pltpu.SemaphoreType.DMA((2 * QUARTERS * tiles,)),
                pltpu.SemaphoreType.DMA((2 * tp,)),
                pltpu.SemaphoreType.DMA((2 * tp,)),
            ],
            compiler_params=pltpu.CompilerParams(
                collective_id=0, has_side_effects=True, vmem_limit_bytes=62 * 2**20),
            name="vocab_head",
        )(hidden.reshape(positions, depth), norm_w, draft_ids, embedding)
        return out[0], out[1]

    return jax.shard_map(local_part, mesh=mesh, in_specs=(P("dp", None, None), P(None), P("tp", None), P("dp", None)), out_specs=(P("dp", None), P("dp", None)), check_vma=False)
```

```python
import functools

import jax
import jax.numpy as jnp
from jax import lax
from jax.experimental import pallas as pl
from jax.experimental.pallas import tpu as pltpu
from jax.sharding import PartitionSpec as P

EPS = 1e-6
MESH = pl.DeviceIdType.MESH
ROWS = 800
HALF = ROWS // 2
SLOTS = 8
SOLO = 8
LANES = 128
SUB = 8
STATS = 4
QUARTERS = 4


def _stats_update(z, first_row, ids, stats):
    top, total, weighted, picked = stats
    rows, width = z.shape
    cube = z.reshape(rows // SUB, SUB, width)
    new_top = jnp.maximum(top, jnp.max(cube, axis=0))
    scale = jnp.exp(top - new_top)
    probs = jnp.exp(cube - new_top[None])
    total = total * scale + jnp.sum(probs, axis=0)
    weighted = weighted * scale + jnp.sum(probs * cube, axis=0)
    row_ids = lax.broadcasted_iota(jnp.int32, (rows, width), 0) + first_row
    hit = jnp.where(row_ids == ids, z, 0.0)
    picked = picked + jnp.sum(hit.reshape(rows // SUB, SUB, width), axis=0)
    return new_top, total, weighted, picked


def _kernel(tp, hidden_hbm, gain_hbm, ids_hbm, emb_hbm, out_ref, hid, gain_vm, ids_vm, wts, outbox, inbox, ring, logits, mine, board,
            hid_sem, gain_sem, ids_sem, ids_sems, ring_sem, hop_send, hop_recv, swap_recv, send_sem, recv_sem):
    me = lax.axis_index("tp")
    group = lax.axis_index("dp")
    parity = lax.rem(group, 2)
    other = group + 1 - 2 * parity
    core = lax.rem(me, 2)
    chip = me // 2
    chips = tp // 2
    shard_rows, depth = emb_hbm.shape
    columns = depth // 2
    pair_chunks = (shard_rows // ROWS - SOLO) // 2
    chunks = SOLO + pair_chunks
    _, seqs, drafts = out_ref.shape
    positions = seqs * drafts
    quarter = positions // QUARTERS
    tiles = quarter // SUB

    hid_copy = pltpu.make_async_copy(hidden_hbm, hid, hid_sem)
    gain_copy = pltpu.make_async_copy(gain_hbm, gain_vm, gain_sem)
    ids_copy = pltpu.make_async_copy(ids_hbm, ids_vm.at[0], ids_sem)
    hid_copy.start(priority=0)
    gain_copy.start(priority=0)
    ids_copy.start(priority=0)

    def first_row(idx):
        return (idx + jnp.where(idx < SOLO, 0, parity * pair_chunks)) * ROWS

    def chunk_copy(idx):
        slot = lax.rem(idx, SLOTS)
        return pltpu.make_async_copy(emb_hbm.at[pl.ds(pl.multiple_of(first_row(idx), ROWS), ROWS)], ring.at[slot], ring_sem.at[slot])

    for idx in range(min(SLOTS, chunks)):
        chunk_copy(idx).start(priority=1)

    own_steps = sorted(range(1, tp), key=lambda step: -min(step, tp - step))
    all_steps = sorted(range(tp), key=lambda step: -min(step, tp - step))
    barrier = pltpu.get_barrier_semaphore()
    for step in own_steps:
        pl.semaphore_signal(barrier, inc=1, device_id={"dp": group, "tp": lax.rem(me + step, tp)}, device_id_type=MESH)
    for step in all_steps:
        pl.semaphore_signal(barrier, inc=1, device_id={"dp": other, "tp": lax.rem(me + step, tp)}, device_id_type=MESH)

    gain_copy.wait()
    hid_copy.wait()
    gain = 1.0 + gain_vm[...].astype(jnp.float32)[None]

    def normalize(x):
        x = x.astype(jnp.float32)
        mean_sq = jnp.sum(x * x, axis=-1, keepdims=True) / depth
        return (x * lax.rsqrt(mean_sq + EPS) * gain).astype(jnp.bfloat16)

    def quarter_of(turn):
        return lax.rem(chip + turn, QUARTERS)

    for turn in (0, 2):
        start = pl.multiple_of(quarter_of(turn) * quarter, quarter)
        outbox[turn // 2] = normalize(hid[pl.ds(start, quarter)]).astype(jnp.float32)

    def spot(turn, tile, side):
        return inbox.at[quarter_of(turn), pl.ds(tile * SUB, SUB), pl.ds(pl.multiple_of(side * columns, columns), columns)]

    def hop(src, turn, tile, side, arrival, device):
        return pltpu.make_async_remote_copy(
            src_ref=src, dst_ref=spot(turn, tile, side), send_sem=hop_send, recv_sem=arrival,
            device_id=device, device_id_type=MESH)

    def across(turn, tile):
        src = outbox.at[turn // 2, pl.ds(tile * SUB, SUB), pl.ds(pl.multiple_of(core * columns, columns), columns)]
        return hop(src, turn, tile, core, hop_recv.at[turn * tiles + tile], {"dp": other, "tp": me})

    def along(tile, up):
        next_chip = lax.rem(chip + (1 if up else chips - 1), chips)
        return hop(spot(0, tile, core), 0, tile, core, hop_recv.at[(3 if up else 1) * tiles + tile], {"dp": group, "tp": 2 * next_chip + core})

    def sideways(turn, tile):
        return hop(spot(turn, tile, core), turn, tile, core, swap_recv, {"dp": group, "tp": me + 1 - 2 * core})

    def landed(turn, tile):
        hop(spot(turn, tile, core), turn, tile, core, hop_recv.at[turn * tiles + tile], {"dp": other, "tp": me}).wait_recv()

    ids_copy.wait()
    pl.semaphore_wait(barrier, 2 * tp - 1)
    for turn in (0, 2):
        for tile in range(tiles):
            across(turn, tile).start()
    ids_hop = pltpu.make_async_remote_copy(
        src_ref=ids_vm.at[0], dst_ref=ids_vm.at[1], send_sem=ids_sems.at[0], recv_sem=ids_sems.at[1],
        device_id={"dp": other, "tp": me}, device_id_type=MESH)
    ids_hop.start()

    wts[:positions] = normalize(hid[...])

    def pass_on(tile):
        landed(0, tile)
        along(tile, True).start()
        along(tile, False).start()

    def swap(turn, tile):
        if turn:
            landed(turn, tile)
        sideways(turn, tile).start()

    agenda = {
        2: [(pass_on, 0)],
        3: [(pass_on, 1)],
        4: [(pass_on, 2), (pass_on, 3)],
        5: [(swap, 0, tile) for tile in range(tiles)],
        6: [(swap, 2, 0), (swap, 2, 1), (swap, 1, 0), (swap, 3, 0)],
        7: [(swap, 1, 1), (swap, 3, 1), (swap, 1, 2), (swap, 3, 2), (swap, 1, 3), (swap, 3, 3), (swap, 2, 2), (swap, 2, 3)],
    }

    def row_ids(which):
        table = ids_vm[which] - me * shard_rows
        return jnp.concatenate([table[seq:seq + 1] for seq in range(seqs)], axis=1)

    own_ids = row_ids(0)
    low = jnp.full((SUB, positions), jnp.finfo(jnp.float32).min, jnp.float32)
    zero = jnp.zeros((SUB, positions), jnp.float32)

    def multiply(idx, width):
        slot = lax.rem(idx, SLOTS)
        stationary = wts[:width]
        for part in range(2):
            rows = slice(part * HALF, (part + 1) * HALF)
            logits[rows, :width] = lax.dot_general(ring[slot, rows], stationary, (((1,), (1,)), ((), ())), preferred_element_type=jnp.float32)

    def refill(idx):
        @pl.when(idx + SLOTS < chunks)
        def _():
            chunk_copy(idx + SLOTS).start(priority=1)

    def reduce(idx, width, ids, stats):
        return _stats_update(logits[:, :width], first_row(idx), ids, stats)

    chunk_copy(0).wait()
    multiply(0, positions)
    refill(0)

    def solo(idx, stats):
        for when, deeds in agenda.items():
            @pl.when(idx == when)
            def _(deeds=deeds):
                for deed, *what in deeds:
                    deed(*what)
        chunk_copy(idx).wait()
        stats = reduce(idx - 1, positions, own_ids, stats)
        multiply(idx, positions)
        refill(idx)
        return stats

    stats = lax.fori_loop(1, SOLO, solo, (low, zero, zero, zero))

    half_box = inbox.at[pl.ds(0, QUARTERS // 2)]
    pltpu.make_async_copy(half_box, half_box, swap_recv).wait()
    ids_hop.wait_recv()
    wts[positions:] = inbox[...].reshape(positions, depth).astype(jnp.bfloat16)
    both_ids = jnp.concatenate([own_ids, row_ids(1)], axis=1)

    chunk_copy(SOLO).wait()
    stats = reduce(SOLO - 1, positions, own_ids, stats)
    multiply(SOLO, 2 * positions)
    refill(SOLO)
    stats = tuple(jnp.concatenate([mine_part, start], axis=1) for mine_part, start in zip(stats, (low, zero, zero, zero)))

    def paired(idx, stats):
        chunk_copy(idx).wait()
        stats = reduce(idx - 1, 2 * positions, both_ids, stats)
        multiply(idx, 2 * positions)
        refill(idx)
        return stats

    stats = lax.fori_loop(SOLO + 1, chunks, paired, stats)
    top, total, weighted, picked = reduce(chunks - 1, 2 * positions, both_ids, stats)

    best = jnp.max(top, axis=0, keepdims=True)
    scale = jnp.exp(top - best)
    summary = (
        best,
        jnp.sum(total * scale, axis=0, keepdims=True),
        jnp.sum(weighted * scale, axis=0, keepdims=True),
        jnp.sum(picked, axis=0, keepdims=True),
    )
    for side in range(2):
        for row, value in enumerate(summary):
            mine[side, row:row + 1] = value[:, side * positions:(side + 1) * positions]

    def report(side, step):
        return pltpu.make_async_remote_copy(
            src_ref=mine.at[side], dst_ref=board.at[side * tp + me], send_sem=send_sem, recv_sem=recv_sem,
            device_id={"dp": other if side else group, "tp": lax.rem(me + step, tp)}, device_id_type=MESH)

    for step in all_steps:
        report(1, step).start()
        if step:
            report(0, step).start()
    board[me] = mine[0]

    ids_hop.wait_send()
    pltpu.make_async_copy(inbox, inbox, hop_send).wait()
    others = board.at[pl.ds(0, 2 * tp - 1)]
    pltpu.make_async_copy(others, others, recv_sem).wait()
    pltpu.make_async_copy(others, others, send_sem).wait()

    every = board[...]
    tops = every[:, 0]
    row_max = jnp.max(tops, axis=0, keepdims=True)
    scale = jnp.exp(tops - row_max)
    exp_total = jnp.sum(every[:, 1] * scale, axis=0, keepdims=True)
    weighted = jnp.sum(every[:, 2] * scale, axis=0, keepdims=True)
    picked = jnp.sum(every[:, 3], axis=0, keepdims=True)
    log_norm = row_max + jnp.log(exp_total)
    log_prob = picked - log_norm
    entropy = log_norm - weighted / exp_total
    for seq in range(seqs):
        lanes = slice(seq * drafts, (seq + 1) * drafts)
        out_ref[0, seq:seq + 1] = log_prob[:, lanes]
        out_ref[1, seq:seq + 1] = entropy[:, lanes]


def solution(mesh):
    tp = mesh.shape["tp"]

    def local_part(hidden, norm_w, embedding, draft_ids):
        seqs, drafts, depth = hidden.shape
        positions = seqs * drafts
        tiles = positions // QUARTERS // SUB
        hbm = pl.BlockSpec(memory_space=pl.ANY)
        out = pl.pallas_call(
            functools.partial(_kernel, tp),
            out_shape=pltpu.VMEM((2, seqs, drafts), jnp.float32),
            in_specs=[hbm] * 4,
            out_specs=pl.BlockSpec(memory_space=pltpu.VMEM),
            scratch_shapes=[
                pltpu.VMEM((positions, depth), jnp.bfloat16),
                pltpu.VMEM((depth,), jnp.bfloat16),
                pltpu.VMEM((2, seqs, drafts), jnp.int32),
                pltpu.VMEM((2 * positions, depth), jnp.bfloat16),
                pltpu.VMEM((2, positions // QUARTERS, depth), jnp.float32),
                pltpu.VMEM((QUARTERS, positions // QUARTERS, depth), jnp.float32),
                pltpu.VMEM((SLOTS, ROWS, depth), jnp.bfloat16),
                pltpu.VMEM((ROWS, 2 * positions), jnp.float32),
                pltpu.VMEM((2, STATS, positions), jnp.float32),
                pltpu.VMEM((2 * tp, STATS, positions), jnp.float32),
                pltpu.SemaphoreType.DMA,
                pltpu.SemaphoreType.DMA,
                pltpu.SemaphoreType.DMA,
                pltpu.SemaphoreType.DMA((2,)),
                pltpu.SemaphoreType.DMA((SLOTS,)),
                pltpu.SemaphoreType.DMA,
                pltpu.SemaphoreType.DMA((QUARTERS * tiles,)),
                pltpu.SemaphoreType.DMA,
                pltpu.SemaphoreType.DMA,
                pltpu.SemaphoreType.DMA,
            ],
            compiler_params=pltpu.CompilerParams(
                collective_id=0, has_side_effects=True, vmem_limit_bytes=62 * 2**20),
            name="vocab_head",
        )(hidden.reshape(positions, depth), norm_w, draft_ids, embedding)
        return out[0], out[1]

    return jax.shard_map(local_part, mesh=mesh, in_specs=(P("dp", None, None), P(None), P("tp", None), P("dp", None)), out_specs=(P("dp", None), P("dp", None)), check_vma=False)
```

```python
import functools

import jax
import jax.numpy as jnp
from jax import lax
from jax.experimental import pallas as pl
from jax.experimental.pallas import tpu as pltpu
from jax.sharding import PartitionSpec as P

EPS = 1e-6
MESH = pl.DeviceIdType.MESH
ROWS = 800
HALF = ROWS // 2
SLOTS = 8
SOLO = 8
LANES = 128
SUB = 8
STATS = 4
QUARTERS = 4


def _stats_update(z, first_row, ids, stats):
    top, total, weighted, picked = stats
    rows, width = z.shape
    cube = z.reshape(rows // SUB, SUB, width)
    new_top = jnp.maximum(top, jnp.max(cube, axis=0))
    scale = jnp.exp(top - new_top)
    probs = jnp.exp(cube - new_top[None])
    total = total * scale + jnp.sum(probs, axis=0)
    weighted = weighted * scale + jnp.sum(probs * cube, axis=0)
    distance = ids - first_row - lax.broadcasted_iota(jnp.int32, (SUB, width), 0)
    for tile in range(rows // SUB):
        picked = jnp.where(distance == tile * SUB, cube[tile], picked)
    return new_top, total, weighted, picked


def _kernel(tp, hidden_hbm, gain_hbm, ids_hbm, emb_hbm, out_ref, hid, gain_vm, ids_vm, wts, outbox, inbox, ring, logits, mine, board,
            hid_sem, gain_sem, ids_sem, ids_sems, ring_sem, hop_send, hop_recv, swap_recv, send_sem, recv_sem):
    me = lax.axis_index("tp")
    group = lax.axis_index("dp")
    parity = lax.rem(group, 2)
    other = group + 1 - 2 * parity
    core = lax.rem(me, 2)
    chip = me // 2
    chips = tp // 2
    shard_rows, depth = emb_hbm.shape
    columns = depth // 2
    pair_chunks = (shard_rows // ROWS - SOLO) // 2
    chunks = SOLO + pair_chunks
    _, seqs, drafts = out_ref.shape
    positions = seqs * drafts
    quarter = positions // QUARTERS
    tiles = quarter // SUB

    hid_copy = pltpu.make_async_copy(hidden_hbm, hid, hid_sem)
    gain_copy = pltpu.make_async_copy(gain_hbm, gain_vm, gain_sem)
    ids_copy = pltpu.make_async_copy(ids_hbm, ids_vm.at[0], ids_sem)
    hid_copy.start(priority=0)
    gain_copy.start(priority=0)
    ids_copy.start(priority=0)

    def first_row(idx):
        return (idx + jnp.where(idx < SOLO, 0, parity * pair_chunks)) * ROWS

    def chunk_copy(idx):
        slot = lax.rem(idx, SLOTS)
        return pltpu.make_async_copy(emb_hbm.at[pl.ds(pl.multiple_of(first_row(idx), ROWS), ROWS)], ring.at[slot], ring_sem.at[slot])

    for idx in range(min(SLOTS, chunks)):
        chunk_copy(idx).start(priority=1)

    own_steps = sorted(range(1, tp), key=lambda step: -min(step, tp - step))
    all_steps = sorted(range(tp), key=lambda step: -min(step, tp - step))
    barrier = pltpu.get_barrier_semaphore()
    for step in own_steps:
        pl.semaphore_signal(barrier, inc=1, device_id={"dp": group, "tp": lax.rem(me + step, tp)}, device_id_type=MESH)
    for step in all_steps:
        pl.semaphore_signal(barrier, inc=1, device_id={"dp": other, "tp": lax.rem(me + step, tp)}, device_id_type=MESH)

    gain_copy.wait()
    hid_copy.wait()
    gain = 1.0 + gain_vm[...].astype(jnp.float32)[None]

    def normalize(x):
        x = x.astype(jnp.float32)
        mean_sq = jnp.sum(x * x, axis=-1, keepdims=True) / depth
        return (x * lax.rsqrt(mean_sq + EPS) * gain).astype(jnp.bfloat16)

    def quarter_of(turn):
        return lax.rem(chip + turn, QUARTERS)

    def prepare(turn):
        start = pl.multiple_of(quarter_of(turn) * quarter, quarter)
        outbox[turn // 2] = normalize(hid[pl.ds(start, quarter)]).astype(jnp.float32)

    prepare(0)

    def spot(turn, tile, side):
        return inbox.at[quarter_of(turn), pl.ds(tile * SUB, SUB), pl.ds(pl.multiple_of(side * columns, columns), columns)]

    def hop(src, turn, tile, side, arrival, device):
        return pltpu.make_async_remote_copy(
            src_ref=src, dst_ref=spot(turn, tile, side), send_sem=hop_send, recv_sem=arrival,
            device_id=device, device_id_type=MESH)

    def across(turn, tile):
        src = outbox.at[turn // 2, pl.ds(tile * SUB, SUB), pl.ds(pl.multiple_of(core * columns, columns), columns)]
        return hop(src, turn, tile, core, hop_recv.at[turn * tiles + tile], {"dp": other, "tp": me})

    def along(tile, up):
        next_chip = lax.rem(chip + (1 if up else chips - 1), chips)
        return hop(spot(0, tile, core), 0, tile, core, hop_recv.at[(3 if up else 1) * tiles + tile], {"dp": group, "tp": 2 * next_chip + core})

    def sideways(turn, tile):
        return hop(spot(turn, tile, core), turn, tile, core, swap_recv, {"dp": group, "tp": me + 1 - 2 * core})

    def landed(turn, tile):
        hop(spot(turn, tile, core), turn, tile, core, hop_recv.at[turn * tiles + tile], {"dp": other, "tp": me}).wait_recv()

    ids_copy.wait()
    pl.semaphore_wait(barrier, 2 * tp - 1)
    for tile in range(tiles):
        across(0, tile).start()
    prepare(2)
    for tile in range(tiles):
        across(2, tile).start()
    ids_hop = pltpu.make_async_remote_copy(
        src_ref=ids_vm.at[0], dst_ref=ids_vm.at[1], send_sem=ids_sems.at[0], recv_sem=ids_sems.at[1],
        device_id={"dp": other, "tp": me}, device_id_type=MESH)
    ids_hop.start()

    wts[:positions] = normalize(hid[...])

    def pass_on(tile):
        landed(0, tile)
        along(tile, True).start()
        along(tile, False).start()

    def swap(turn, tile):
        if turn:
            landed(turn, tile)
        sideways(turn, tile).start()

    agenda = {
        2: [(pass_on, 0)],
        3: [(pass_on, 1)],
        4: [(pass_on, 2), (pass_on, 3)],
        5: [(swap, 0, tile) for tile in range(tiles)],
        6: [(swap, 2, 0), (swap, 2, 1), (swap, 1, 0), (swap, 3, 0)],
        7: [(swap, 1, 1), (swap, 3, 1), (swap, 1, 2), (swap, 3, 2), (swap, 1, 3), (swap, 3, 3), (swap, 2, 2), (swap, 2, 3)],
    }

    def row_ids(which):
        table = ids_vm[which] - me * shard_rows
        return jnp.concatenate([table[seq:seq + 1] for seq in range(seqs)], axis=1)

    own_ids = row_ids(0)
    low = jnp.full((SUB, positions), jnp.finfo(jnp.float32).min, jnp.float32)
    zero = jnp.zeros((SUB, positions), jnp.float32)

    def multiply(idx, width):
        slot = lax.rem(idx, SLOTS)
        stationary = wts[:width]
        for part in range(2):
            rows = slice(part * HALF, (part + 1) * HALF)
            logits[rows, :width] = lax.dot_general(ring[slot, rows], stationary, (((1,), (1,)), ((), ())), preferred_element_type=jnp.float32)

    def refill(idx):
        @pl.when(idx + SLOTS < chunks)
        def _():
            chunk_copy(idx + SLOTS).start(priority=1)

    def reduce(idx, width, ids, stats):
        return _stats_update(logits[:, :width], first_row(idx), ids, stats)

    chunk_copy(0).wait()
    multiply(0, positions)
    refill(0)

    def solo(idx, stats):
        for when, deeds in agenda.items():
            @pl.when(idx == when)
            def _(deeds=deeds):
                for deed, *what in deeds:
                    deed(*what)
        chunk_copy(idx).wait()
        stats = reduce(idx - 1, positions, own_ids, stats)
        multiply(idx, positions)
        refill(idx)
        return stats

    stats = lax.fori_loop(1, SOLO, solo, (low, zero, zero, zero))

    half_box = inbox.at[pl.ds(0, QUARTERS // 2)]
    pltpu.make_async_copy(half_box, half_box, swap_recv).wait()
    ids_hop.wait_recv()
    wts[positions:] = inbox[...].reshape(positions, depth).astype(jnp.bfloat16)
    both_ids = jnp.concatenate([own_ids, row_ids(1)], axis=1)

    chunk_copy(SOLO).wait()
    stats = reduce(SOLO - 1, positions, own_ids, stats)
    multiply(SOLO, 2 * positions)
    refill(SOLO)
    stats = tuple(jnp.concatenate([mine_part, start], axis=1) for mine_part, start in zip(stats, (low, zero, zero, zero)))

    def paired(idx, stats):
        chunk_copy(idx).wait()
        stats = reduce(idx - 1, 2 * positions, both_ids, stats)
        multiply(idx, 2 * positions)
        refill(idx)
        return stats

    stats = lax.fori_loop(SOLO + 1, chunks, paired, stats)
    top, total, weighted, picked = reduce(chunks - 1, 2 * positions, both_ids, stats)

    best = jnp.max(top, axis=0, keepdims=True)
    scale = jnp.exp(top - best)
    summary = (
        best,
        jnp.sum(total * scale, axis=0, keepdims=True),
        jnp.sum(weighted * scale, axis=0, keepdims=True),
        jnp.sum(picked, axis=0, keepdims=True),
    )
    for side in range(2):
        for row, value in enumerate(summary):
            mine[side, row:row + 1] = value[:, side * positions:(side + 1) * positions]

    def report(side, step):
        return pltpu.make_async_remote_copy(
            src_ref=mine.at[side], dst_ref=board.at[side * tp + me], send_sem=send_sem, recv_sem=recv_sem,
            device_id={"dp": other if side else group, "tp": lax.rem(me + step, tp)}, device_id_type=MESH)

    for step in all_steps:
        report(1, step).start()
        if step:
            report(0, step).start()
    board[me] = mine[0]

    ids_hop.wait_send()
    pltpu.make_async_copy(inbox, inbox, hop_send).wait()
    others = board.at[pl.ds(0, 2 * tp - 1)]
    pltpu.make_async_copy(others, others, recv_sem).wait()
    pltpu.make_async_copy(others, others, send_sem).wait()

    every = board[...]
    tops = every[:, 0]
    row_max = jnp.max(tops, axis=0, keepdims=True)
    scale = jnp.exp(tops - row_max)
    exp_total = jnp.sum(every[:, 1] * scale, axis=0, keepdims=True)
    weighted = jnp.sum(every[:, 2] * scale, axis=0, keepdims=True)
    picked = jnp.sum(every[:, 3], axis=0, keepdims=True)
    log_norm = row_max + jnp.log(exp_total)
    log_prob = picked - log_norm
    entropy = log_norm - weighted / exp_total
    for seq in range(seqs):
        lanes = slice(seq * drafts, (seq + 1) * drafts)
        out_ref[0, seq:seq + 1] = log_prob[:, lanes]
        out_ref[1, seq:seq + 1] = entropy[:, lanes]


def solution(mesh):
    tp = mesh.shape["tp"]

    def local_part(hidden, norm_w, embedding, draft_ids):
        seqs, drafts, depth = hidden.shape
        positions = seqs * drafts
        tiles = positions // QUARTERS // SUB
        hbm = pl.BlockSpec(memory_space=pl.ANY)
        out = pl.pallas_call(
            functools.partial(_kernel, tp),
            out_shape=pltpu.VMEM((2, seqs, drafts), jnp.float32),
            in_specs=[hbm] * 4,
            out_specs=pl.BlockSpec(memory_space=pltpu.VMEM),
            scratch_shapes=[
                pltpu.VMEM((positions, depth), jnp.bfloat16),
                pltpu.VMEM((depth,), jnp.bfloat16),
                pltpu.VMEM((2, seqs, drafts), jnp.int32),
                pltpu.VMEM((2 * positions, depth), jnp.bfloat16),
                pltpu.VMEM((2, positions // QUARTERS, depth), jnp.float32),
                pltpu.VMEM((QUARTERS, positions // QUARTERS, depth), jnp.float32),
                pltpu.VMEM((SLOTS, ROWS, depth), jnp.bfloat16),
                pltpu.VMEM((ROWS, 2 * positions), jnp.float32),
                pltpu.VMEM((2, STATS, positions), jnp.float32),
                pltpu.VMEM((2 * tp, STATS, positions), jnp.float32),
                pltpu.SemaphoreType.DMA,
                pltpu.SemaphoreType.DMA,
                pltpu.SemaphoreType.DMA,
                pltpu.SemaphoreType.DMA((2,)),
                pltpu.SemaphoreType.DMA((SLOTS,)),
                pltpu.SemaphoreType.DMA,
                pltpu.SemaphoreType.DMA((QUARTERS * tiles,)),
                pltpu.SemaphoreType.DMA,
                pltpu.SemaphoreType.DMA,
                pltpu.SemaphoreType.DMA,
            ],
            compiler_params=pltpu.CompilerParams(
                collective_id=0, has_side_effects=True, vmem_limit_bytes=62 * 2**20),
            name="vocab_head",
        )(hidden.reshape(positions, depth), norm_w, draft_ids, embedding)
        return out[0], out[1]

    return jax.shard_map(local_part, mesh=mesh, in_specs=(P("dp", None, None), P(None), P("tp", None), P("dp", None)), out_specs=(P("dp", None), P("dp", None)), check_vma=False)
```

```python
import functools

import jax
import jax.numpy as jnp
from jax import lax
from jax.experimental import pallas as pl
from jax.experimental.pallas import tpu as pltpu
from jax.sharding import PartitionSpec as P

EPS = 1e-6
MESH = pl.DeviceIdType.MESH
SOLO_ROWS = 800
SOLO = 8
PAIR_ROWS = 832
PAIRS = 6
LANES = 128
SUB = 8
STATS = 4
QUARTERS = 4


def _stats_update(z, first_row, ids, stats):
    top, total, weighted, picked = stats
    rows, width = z.shape
    cube = z.reshape(rows // SUB, SUB, width)
    new_top = jnp.maximum(top, jnp.max(cube, axis=0))
    scale = jnp.exp(top - new_top)
    probs = jnp.exp(cube - new_top[None])
    total = total * scale + jnp.sum(probs, axis=0)
    weighted = weighted * scale + jnp.sum(probs * cube, axis=0)
    distance = ids - first_row - lax.broadcasted_iota(jnp.int32, (SUB, width), 0)
    for tile in range(rows // SUB):
        picked = jnp.where(distance == tile * SUB, cube[tile], picked)
    return new_top, total, weighted, picked


def _kernel(tp, hidden_hbm, gain_hbm, ids_hbm, emb_hbm, out_ref, hid, gain_vm, ids_vm, wts, outbox, inbox, ring, logits, mine, board,
            hid_sem, gain_sem, ids_sem, ids_sems, ring_sem, hop_send, hop_recv, swap_recv, send_sem, recv_sem):
    me = lax.axis_index("tp")
    group = lax.axis_index("dp")
    parity = lax.rem(group, 2)
    other = group + 1 - 2 * parity
    core = lax.rem(me, 2)
    chip = me // 2
    chips = tp // 2
    shard_rows, depth = emb_hbm.shape
    columns = depth // 2
    pair_base = shard_rows - 2 * PAIRS * PAIR_ROWS
    lead_rows = pair_base - (SOLO - 1) * SOLO_ROWS
    _, seqs, drafts = out_ref.shape
    positions = seqs * drafts
    quarter = positions // QUARTERS
    tiles = quarter // SUB

    hid_copy = pltpu.make_async_copy(hidden_hbm, hid, hid_sem)
    gain_copy = pltpu.make_async_copy(gain_hbm, gain_vm, gain_sem)
    ids_copy = pltpu.make_async_copy(ids_hbm, ids_vm.at[0], ids_sem)
    hid_copy.start(priority=0)
    gain_copy.start(priority=0)
    ids_copy.start(priority=0)

    def solo_row(idx):
        return lead_rows + (idx - 1) * SOLO_ROWS

    def pair_row(idx):
        return pair_base + (parity * PAIRS + idx) * PAIR_ROWS

    def fetch(row, rows, slot):
        return pltpu.make_async_copy(emb_hbm.at[pl.ds(pl.multiple_of(row, 32), rows)], ring.at[slot, pl.ds(0, rows)], ring_sem.at[slot])

    def fetch_solo(idx):
        return fetch(solo_row(idx), SOLO_ROWS, idx)

    def fetch_pair(idx):
        return fetch(pair_row(idx), PAIR_ROWS, idx)

    fetch_lead = fetch(0, lead_rows, 0)
    fetch_lead.start(priority=1)
    for idx in range(1, SOLO):
        fetch_solo(idx).start(priority=1)

    own_steps = sorted(range(1, tp), key=lambda step: -min(step, tp - step))
    all_steps = sorted(range(tp), key=lambda step: -min(step, tp - step))
    barrier = pltpu.get_barrier_semaphore()
    for step in own_steps:
        pl.semaphore_signal(barrier, inc=1, device_id={"dp": group, "tp": lax.rem(me + step, tp)}, device_id_type=MESH)
    for step in all_steps:
        pl.semaphore_signal(barrier, inc=1, device_id={"dp": other, "tp": lax.rem(me + step, tp)}, device_id_type=MESH)

    gain_copy.wait()
    hid_copy.wait()
    gain = 1.0 + gain_vm[...].astype(jnp.float32)[None]

    def normalize(x):
        x = x.astype(jnp.float32)
        mean_sq = jnp.sum(x * x, axis=-1, keepdims=True) / depth
        return (x * lax.rsqrt(mean_sq + EPS) * gain).astype(jnp.bfloat16)

    def quarter_of(turn):
        return lax.rem(chip + turn, QUARTERS)

    def prepare(turn):
        start = pl.multiple_of(quarter_of(turn) * quarter, quarter)
        outbox[turn // 2] = normalize(hid[pl.ds(start, quarter)]).astype(jnp.float32)

    prepare(0)

    def spot(turn, tile, side):
        return inbox.at[quarter_of(turn), pl.ds(tile * SUB, SUB), pl.ds(pl.multiple_of(side * columns, columns), columns)]

    def hop(src, turn, tile, side, arrival, device):
        return pltpu.make_async_remote_copy(
            src_ref=src, dst_ref=spot(turn, tile, side), send_sem=hop_send, recv_sem=arrival,
            device_id=device, device_id_type=MESH)

    def across(turn, tile):
        src = outbox.at[turn // 2, pl.ds(tile * SUB, SUB), pl.ds(pl.multiple_of(core * columns, columns), columns)]
        return hop(src, turn, tile, core, hop_recv.at[turn * tiles + tile], {"dp": other, "tp": me})

    def along(tile, up):
        next_chip = lax.rem(chip + (1 if up else chips - 1), chips)
        return hop(spot(0, tile, core), 0, tile, core, hop_recv.at[(3 if up else 1) * tiles + tile], {"dp": group, "tp": 2 * next_chip + core})

    def sideways(turn, tile):
        return hop(spot(turn, tile, core), turn, tile, core, swap_recv, {"dp": group, "tp": me + 1 - 2 * core})

    def landed(turn, tile):
        hop(spot(turn, tile, core), turn, tile, core, hop_recv.at[turn * tiles + tile], {"dp": other, "tp": me}).wait_recv()

    ids_copy.wait()
    pl.semaphore_wait(barrier, 2 * tp - 1)
    for tile in range(tiles):
        across(0, tile).start()
    prepare(2)
    for tile in range(tiles):
        across(2, tile).start()
    ids_hop = pltpu.make_async_remote_copy(
        src_ref=ids_vm.at[0], dst_ref=ids_vm.at[1], send_sem=ids_sems.at[0], recv_sem=ids_sems.at[1],
        device_id={"dp": other, "tp": me}, device_id_type=MESH)
    ids_hop.start()

    wts[:positions] = normalize(hid[...])

    def pass_on(tile):
        landed(0, tile)
        along(tile, True).start()
        along(tile, False).start()

    def swap(turn, tile):
        if turn:
            landed(turn, tile)
        sideways(turn, tile).start()

    agenda = {
        3: [(pass_on, 0)],
        4: [(pass_on, 1), (pass_on, 2)],
        5: [(pass_on, 3), (swap, 0, 0), (swap, 0, 1), (swap, 0, 2)],
        6: [(swap, 0, 3), (swap, 2, 0), (swap, 2, 1), (swap, 1, 0), (swap, 3, 0)],
        7: [(swap, 1, 1), (swap, 3, 1), (swap, 1, 2), (swap, 3, 2), (swap, 2, 2), (swap, 1, 3), (swap, 3, 3), (swap, 2, 3)],
    }

    def row_ids(which):
        table = ids_vm[which] - me * shard_rows
        return jnp.concatenate([table[seq:seq + 1] for seq in range(seqs)], axis=1)

    own_ids = row_ids(0)
    low = jnp.full((SUB, positions), jnp.finfo(jnp.float32).min, jnp.float32)
    zero = jnp.zeros((SUB, positions), jnp.float32)

    def multiply(slot, rows, width):
        stationary = wts[:width]
        half = rows // 2
        for part in range(2):
            span = slice(part * half, (part + 1) * half)
            logits[span, :width] = lax.dot_general(ring[slot, span], stationary, (((1,), (1,)), ((), ())), preferred_element_type=jnp.float32)

    def reduce(row, rows, width, ids, stats):
        return _stats_update(logits[:rows, :width], row, ids, stats)

    fetch_lead.wait()
    multiply(0, lead_rows, positions)
    fetch_pair(0).start(priority=1)

    fetch_solo(1).wait()
    stats = reduce(0, lead_rows, positions, own_ids, (low, zero, zero, zero))
    multiply(1, SOLO_ROWS, positions)
    fetch_pair(1).start(priority=1)

    def solo(idx, stats):
        for when, deeds in agenda.items():
            @pl.when(idx == when)
            def _(deeds=deeds):
                for deed, *what in deeds:
                    deed(*what)
        fetch_solo(idx).wait()
        stats = reduce(solo_row(idx - 1), SOLO_ROWS, positions, own_ids, stats)
        multiply(idx, SOLO_ROWS, positions)

        @pl.when(idx < PAIRS)
        def _():
            fetch_pair(idx).start(priority=1)

        return stats

    stats = lax.fori_loop(2, SOLO, solo, stats)

    half_box = inbox.at[pl.ds(0, QUARTERS // 2)]
    pltpu.make_async_copy(half_box, half_box, swap_recv).wait()
    ids_hop.wait_recv()
    wts[positions:] = inbox[...].reshape(positions, depth).astype(jnp.bfloat16)
    both_ids = jnp.concatenate([own_ids, row_ids(1)], axis=1)

    fetch_pair(0).wait()
    stats = reduce(solo_row(SOLO - 1), SOLO_ROWS, positions, own_ids, stats)
    multiply(0, PAIR_ROWS, 2 * positions)
    stats = tuple(jnp.concatenate([mine_part, start], axis=1) for mine_part, start in zip(stats, (low, zero, zero, zero)))

    def paired(idx, stats):
        fetch_pair(idx).wait()
        stats = reduce(pair_row(idx - 1), PAIR_ROWS, 2 * positions, both_ids, stats)
        multiply(idx, PAIR_ROWS, 2 * positions)
        return stats

    stats = lax.fori_loop(1, PAIRS, paired, stats)
    top, total, weighted, picked = reduce(pair_row(PAIRS - 1), PAIR_ROWS, 2 * positions, both_ids, stats)

    best = jnp.max(top, axis=0, keepdims=True)
    scale = jnp.exp(top - best)
    summary = (
        best,
        jnp.sum(total * scale, axis=0, keepdims=True),
        jnp.sum(weighted * scale, axis=0, keepdims=True),
        jnp.sum(picked, axis=0, keepdims=True),
    )
    for side in range(2):
        for row, value in enumerate(summary):
            mine[side, row:row + 1] = value[:, side * positions:(side + 1) * positions]

    def report(side, step):
        return pltpu.make_async_remote_copy(
            src_ref=mine.at[side], dst_ref=board.at[side * tp + me], send_sem=send_sem, recv_sem=recv_sem,
            device_id={"dp": other if side else group, "tp": lax.rem(me + step, tp)}, device_id_type=MESH)

    for step in all_steps:
        report(1, step).start()
        if step:
            report(0, step).start()
    board[me] = mine[0]

    ids_hop.wait_send()
    pltpu.make_async_copy(inbox, inbox, hop_send).wait()
    others = board.at[pl.ds(0, 2 * tp - 1)]
    pltpu.make_async_copy(others, others, recv_sem).wait()
    pltpu.make_async_copy(others, others, send_sem).wait()

    every = board[...]
    tops = every[:, 0]
    row_max = jnp.max(tops, axis=0, keepdims=True)
    scale = jnp.exp(tops - row_max)
    exp_total = jnp.sum(every[:, 1] * scale, axis=0, keepdims=True)
    weighted = jnp.sum(every[:, 2] * scale, axis=0, keepdims=True)
    picked = jnp.sum(every[:, 3], axis=0, keepdims=True)
    log_norm = row_max + jnp.log(exp_total)
    log_prob = picked - log_norm
    entropy = log_norm - weighted / exp_total
    for seq in range(seqs):
        lanes = slice(seq * drafts, (seq + 1) * drafts)
        out_ref[0, seq:seq + 1] = log_prob[:, lanes]
        out_ref[1, seq:seq + 1] = entropy[:, lanes]


def solution(mesh):
    tp = mesh.shape["tp"]

    def local_part(hidden, norm_w, embedding, draft_ids):
        seqs, drafts, depth = hidden.shape
        positions = seqs * drafts
        tiles = positions // QUARTERS // SUB
        hbm = pl.BlockSpec(memory_space=pl.ANY)
        out = pl.pallas_call(
            functools.partial(_kernel, tp),
            out_shape=pltpu.VMEM((2, seqs, drafts), jnp.float32),
            in_specs=[hbm] * 4,
            out_specs=pl.BlockSpec(memory_space=pltpu.VMEM),
            scratch_shapes=[
                pltpu.VMEM((positions, depth), jnp.bfloat16),
                pltpu.VMEM((depth,), jnp.bfloat16),
                pltpu.VMEM((2, seqs, drafts), jnp.int32),
                pltpu.VMEM((2 * positions, depth), jnp.bfloat16),
                pltpu.VMEM((2, positions // QUARTERS, depth), jnp.float32),
                pltpu.VMEM((QUARTERS, positions // QUARTERS, depth), jnp.float32),
                pltpu.VMEM((SOLO, PAIR_ROWS, depth), jnp.bfloat16),
                pltpu.VMEM((PAIR_ROWS, 2 * positions), jnp.float32),
                pltpu.VMEM((2, STATS, positions), jnp.float32),
                pltpu.VMEM((2 * tp, STATS, positions), jnp.float32),
                pltpu.SemaphoreType.DMA,
                pltpu.SemaphoreType.DMA,
                pltpu.SemaphoreType.DMA,
                pltpu.SemaphoreType.DMA((2,)),
                pltpu.SemaphoreType.DMA((SOLO,)),
                pltpu.SemaphoreType.DMA,
                pltpu.SemaphoreType.DMA((QUARTERS * tiles,)),
                pltpu.SemaphoreType.DMA,
                pltpu.SemaphoreType.DMA,
                pltpu.SemaphoreType.DMA,
            ],
            compiler_params=pltpu.CompilerParams(
                collective_id=0, has_side_effects=True, vmem_limit_bytes=62 * 2**20),
            name="vocab_head",
        )(hidden.reshape(positions, depth), norm_w, draft_ids, embedding)
        return out[0], out[1]

    return jax.shard_map(local_part, mesh=mesh, in_specs=(P("dp", None, None), P(None), P("tp", None), P("dp", None)), out_specs=(P("dp", None), P("dp", None)), check_vma=False)
```

```python
import functools

import jax
import jax.numpy as jnp
from jax import lax
from jax.experimental import pallas as pl
from jax.experimental.pallas import tpu as pltpu
from jax.sharding import PartitionSpec as P

EPS = 1e-6
MESH = pl.DeviceIdType.MESH
SOLO_ROWS = 800
SOLO = 8
PAIR_ROWS = 832
PAIRS = 6
LANES = 128
SUB = 8
STATS = 4
QUARTERS = 4
ROUNDS = 5


def _stats_update(z, first_row, ids, stats):
    top, total, weighted, picked = stats
    rows, width = z.shape
    cube = z.reshape(rows // SUB, SUB, width)
    new_top = jnp.maximum(top, jnp.max(cube, axis=0))
    scale = jnp.exp(top - new_top)
    probs = jnp.exp(cube - new_top[None])
    total = total * scale + jnp.sum(probs, axis=0)
    weighted = weighted * scale + jnp.sum(probs * cube, axis=0)
    distance = ids - first_row - lax.broadcasted_iota(jnp.int32, (SUB, width), 0)
    for tile in range(rows // SUB):
        picked = jnp.where(distance == tile * SUB, cube[tile], picked)
    return new_top, total, weighted, picked


def _kernel(tp, hidden_hbm, gain_hbm, ids_hbm, emb_hbm, out_ref, hid, gain_vm, ids_vm, wts, outbox, inbox, ring, logits, mine, board,
            hid_sem, gain_sem, ids_sem, ids_sems, ring_sem, hop_send, hop_recv, swap_recv, send_sem, recv_sem, round_sem):
    me = lax.axis_index("tp")
    group = lax.axis_index("dp")
    parity = lax.rem(group, 2)
    other = group + 1 - 2 * parity
    core = lax.rem(me, 2)
    chip = me // 2
    chips = tp // 2
    shard_rows, depth = emb_hbm.shape
    columns = depth // 2
    pair_base = shard_rows - 2 * PAIRS * PAIR_ROWS
    lead_rows = pair_base - (SOLO - 1) * SOLO_ROWS
    _, seqs, drafts = out_ref.shape
    positions = seqs * drafts
    quarter = positions // QUARTERS
    tiles = quarter // SUB

    hid_copy = pltpu.make_async_copy(hidden_hbm, hid, hid_sem)
    gain_copy = pltpu.make_async_copy(gain_hbm, gain_vm, gain_sem)
    ids_copy = pltpu.make_async_copy(ids_hbm, ids_vm.at[0], ids_sem)
    hid_copy.start(priority=0)
    gain_copy.start(priority=0)
    ids_copy.start(priority=0)

    def solo_row(idx):
        return lead_rows + (idx - 1) * SOLO_ROWS

    def pair_row(idx):
        return pair_base + (parity * PAIRS + idx) * PAIR_ROWS

    def fetch(row, rows, slot):
        return pltpu.make_async_copy(emb_hbm.at[pl.ds(pl.multiple_of(row, 32), rows)], ring.at[slot, pl.ds(0, rows)], ring_sem.at[slot])

    def fetch_solo(idx):
        return fetch(solo_row(idx), SOLO_ROWS, idx)

    def fetch_pair(idx):
        return fetch(pair_row(idx), PAIR_ROWS, idx)

    fetch_lead = fetch(0, lead_rows, 0)
    fetch_lead.start(priority=1)
    for idx in range(1, SOLO):
        fetch_solo(idx).start(priority=1)

    all_steps = sorted(range(tp), key=lambda step: -min(step, tp - step))
    upper, lower = (2 * lax.rem(chip + shift, chips) + core for shift in (1, chips - 1))
    neighbours = (
        {"dp": other, "tp": me},
        {"dp": group, "tp": me + 1 - 2 * core},
        {"dp": group, "tp": upper},
        {"dp": group, "tp": lower},
    )

    def greet(semaphore):
        for device in neighbours:
            pl.semaphore_signal(semaphore, inc=1, device_id=device, device_id_type=MESH)

    def meet(turn):
        pl.semaphore_wait(round_sem.at[turn], len(neighbours))
        if turn + 1 < ROUNDS:
            greet(round_sem.at[turn + 1])

    barrier = pltpu.get_barrier_semaphore()
    greet(barrier)

    gain_copy.wait()
    hid_copy.wait()
    gain = 1.0 + gain_vm[...].astype(jnp.float32)[None]

    def normalize(x):
        x = x.astype(jnp.float32)
        mean_sq = jnp.sum(x * x, axis=-1, keepdims=True) / depth
        return (x * lax.rsqrt(mean_sq + EPS) * gain).astype(jnp.bfloat16)

    def quarter_of(turn):
        return lax.rem(chip + turn, QUARTERS)

    def prepare(turn):
        start = pl.multiple_of(quarter_of(turn) * quarter, quarter)
        outbox[turn // 2] = normalize(hid[pl.ds(start, quarter)]).astype(jnp.float32)

    prepare(0)

    def spot(turn, tile, side):
        return inbox.at[quarter_of(turn), pl.ds(tile * SUB, SUB), pl.ds(pl.multiple_of(side * columns, columns), columns)]

    def hop(src, turn, tile, side, arrival, device):
        return pltpu.make_async_remote_copy(
            src_ref=src, dst_ref=spot(turn, tile, side), send_sem=hop_send, recv_sem=arrival,
            device_id=device, device_id_type=MESH)

    def across(turn, tile):
        src = outbox.at[turn // 2, pl.ds(tile * SUB, SUB), pl.ds(pl.multiple_of(core * columns, columns), columns)]
        return hop(src, turn, tile, core, hop_recv.at[turn * tiles + tile], {"dp": other, "tp": me})

    def along(tile, up):
        return hop(spot(0, tile, core), 0, tile, core, hop_recv.at[(3 if up else 1) * tiles + tile], {"dp": group, "tp": upper if up else lower})

    def sideways(turn, tile):
        return hop(spot(turn, tile, core), turn, tile, core, swap_recv, {"dp": group, "tp": me + 1 - 2 * core})

    def landed(turn, tile):
        hop(spot(turn, tile, core), turn, tile, core, hop_recv.at[turn * tiles + tile], {"dp": other, "tp": me}).wait_recv()

    ids_copy.wait()
    pl.semaphore_wait(barrier, len(neighbours))
    greet(round_sem.at[0])
    for tile in range(tiles):
        across(0, tile).start()
    prepare(2)
    for tile in range(tiles):
        across(2, tile).start()
    ids_hop = pltpu.make_async_remote_copy(
        src_ref=ids_vm.at[0], dst_ref=ids_vm.at[1], send_sem=ids_sems.at[0], recv_sem=ids_sems.at[1],
        device_id={"dp": other, "tp": me}, device_id_type=MESH)
    ids_hop.start()

    wts[:positions] = normalize(hid[...])

    def pass_on(tile):
        landed(0, tile)
        along(tile, True).start()
        along(tile, False).start()

    def swap(turn, tile):
        if turn:
            landed(turn, tile)
        sideways(turn, tile).start()

    agenda = {
        3: [(pass_on, 0), (meet, 0)],
        4: [(pass_on, 1), (pass_on, 2)],
        5: [(pass_on, 3), (swap, 0, 0), (swap, 0, 1), (swap, 0, 2), (meet, 1)],
        6: [(swap, 0, 3), (swap, 2, 0), (swap, 2, 1), (swap, 1, 0), (swap, 3, 0)],
        7: [(swap, 1, 1), (swap, 3, 1), (swap, 1, 2), (swap, 3, 2), (swap, 2, 2), (swap, 1, 3), (swap, 3, 3), (swap, 2, 3), (meet, 2)],
    }

    def row_ids(which):
        table = ids_vm[which] - me * shard_rows
        return jnp.concatenate([table[seq:seq + 1] for seq in range(seqs)], axis=1)

    own_ids = row_ids(0)
    low = jnp.full((SUB, positions), jnp.finfo(jnp.float32).min, jnp.float32)
    zero = jnp.zeros((SUB, positions), jnp.float32)

    def multiply(slot, rows, width):
        stationary = wts[:width]
        half = rows // 2
        for part in range(2):
            span = slice(part * half, (part + 1) * half)
            logits[span, :width] = lax.dot_general(ring[slot, span], stationary, (((1,), (1,)), ((), ())), preferred_element_type=jnp.float32)

    def reduce(row, rows, width, ids, stats):
        return _stats_update(logits[:rows, :width], row, ids, stats)

    fetch_lead.wait()
    multiply(0, lead_rows, positions)
    fetch_pair(0).start(priority=1)

    fetch_solo(1).wait()
    stats = reduce(0, lead_rows, positions, own_ids, (low, zero, zero, zero))
    multiply(1, SOLO_ROWS, positions)
    fetch_pair(1).start(priority=1)

    def solo(idx, stats):
        for when, deeds in agenda.items():
            @pl.when(idx == when)
            def _(deeds=deeds):
                for deed, *what in deeds:
                    deed(*what)
        fetch_solo(idx).wait()
        stats = reduce(solo_row(idx - 1), SOLO_ROWS, positions, own_ids, stats)
        multiply(idx, SOLO_ROWS, positions)

        @pl.when(idx < PAIRS)
        def _():
            fetch_pair(idx).start(priority=1)

        return stats

    stats = lax.fori_loop(2, SOLO, solo, stats)

    half_box = inbox.at[pl.ds(0, QUARTERS // 2)]
    pltpu.make_async_copy(half_box, half_box, swap_recv).wait()
    ids_hop.wait_recv()
    wts[positions:] = inbox[...].reshape(positions, depth).astype(jnp.bfloat16)
    both_ids = jnp.concatenate([own_ids, row_ids(1)], axis=1)

    fetch_pair(0).wait()
    stats = reduce(solo_row(SOLO - 1), SOLO_ROWS, positions, own_ids, stats)
    multiply(0, PAIR_ROWS, 2 * positions)
    stats = tuple(jnp.concatenate([mine_part, start], axis=1) for mine_part, start in zip(stats, (low, zero, zero, zero)))

    def paired(idx, stats):
        for turn in range(3, ROUNDS):
            @pl.when(idx == 2 * turn - 4)
            def _(turn=turn):
                meet(turn)
        fetch_pair(idx).wait()
        stats = reduce(pair_row(idx - 1), PAIR_ROWS, 2 * positions, both_ids, stats)
        multiply(idx, PAIR_ROWS, 2 * positions)
        return stats

    stats = lax.fori_loop(1, PAIRS, paired, stats)
    top, total, weighted, picked = reduce(pair_row(PAIRS - 1), PAIR_ROWS, 2 * positions, both_ids, stats)

    best = jnp.max(top, axis=0, keepdims=True)
    scale = jnp.exp(top - best)
    summary = (
        best,
        jnp.sum(total * scale, axis=0, keepdims=True),
        jnp.sum(weighted * scale, axis=0, keepdims=True),
        jnp.sum(picked, axis=0, keepdims=True),
    )
    for side in range(2):
        for row, value in enumerate(summary):
            mine[side, row:row + 1] = value[:, side * positions:(side + 1) * positions]

    def report(side, step):
        return pltpu.make_async_remote_copy(
            src_ref=mine.at[side], dst_ref=board.at[side * tp + me], send_sem=send_sem, recv_sem=recv_sem,
            device_id={"dp": other if side else group, "tp": lax.rem(me + step, tp)}, device_id_type=MESH)

    for step in all_steps:
        report(1, step).start()
        if step:
            report(0, step).start()
    board[me] = mine[0]

    ids_hop.wait_send()
    pltpu.make_async_copy(inbox, inbox, hop_send).wait()
    others = board.at[pl.ds(0, 2 * tp - 1)]
    pltpu.make_async_copy(others, others, recv_sem).wait()
    pltpu.make_async_copy(others, others, send_sem).wait()

    every = board[...]
    tops = every[:, 0]
    row_max = jnp.max(tops, axis=0, keepdims=True)
    scale = jnp.exp(tops - row_max)
    exp_total = jnp.sum(every[:, 1] * scale, axis=0, keepdims=True)
    weighted = jnp.sum(every[:, 2] * scale, axis=0, keepdims=True)
    picked = jnp.sum(every[:, 3], axis=0, keepdims=True)
    log_norm = row_max + jnp.log(exp_total)
    log_prob = picked - log_norm
    entropy = log_norm - weighted / exp_total
    for seq in range(seqs):
        lanes = slice(seq * drafts, (seq + 1) * drafts)
        out_ref[0, seq:seq + 1] = log_prob[:, lanes]
        out_ref[1, seq:seq + 1] = entropy[:, lanes]


def solution(mesh):
    tp = mesh.shape["tp"]

    def local_part(hidden, norm_w, embedding, draft_ids):
        seqs, drafts, depth = hidden.shape
        positions = seqs * drafts
        tiles = positions // QUARTERS // SUB
        hbm = pl.BlockSpec(memory_space=pl.ANY)
        out = pl.pallas_call(
            functools.partial(_kernel, tp),
            out_shape=pltpu.VMEM((2, seqs, drafts), jnp.float32),
            in_specs=[hbm] * 4,
            out_specs=pl.BlockSpec(memory_space=pltpu.VMEM),
            scratch_shapes=[
                pltpu.VMEM((positions, depth), jnp.bfloat16),
                pltpu.VMEM((depth,), jnp.bfloat16),
                pltpu.VMEM((2, seqs, drafts), jnp.int32),
                pltpu.VMEM((2 * positions, depth), jnp.bfloat16),
                pltpu.VMEM((2, positions // QUARTERS, depth), jnp.float32),
                pltpu.VMEM((QUARTERS, positions // QUARTERS, depth), jnp.float32),
                pltpu.VMEM((SOLO, PAIR_ROWS, depth), jnp.bfloat16),
                pltpu.VMEM((PAIR_ROWS, 2 * positions), jnp.float32),
                pltpu.VMEM((2, STATS, positions), jnp.float32),
                pltpu.VMEM((2 * tp, STATS, positions), jnp.float32),
                pltpu.SemaphoreType.DMA,
                pltpu.SemaphoreType.DMA,
                pltpu.SemaphoreType.DMA,
                pltpu.SemaphoreType.DMA((2,)),
                pltpu.SemaphoreType.DMA((SOLO,)),
                pltpu.SemaphoreType.DMA,
                pltpu.SemaphoreType.DMA((QUARTERS * tiles,)),
                pltpu.SemaphoreType.DMA,
                pltpu.SemaphoreType.DMA,
                pltpu.SemaphoreType.DMA,
                pltpu.SemaphoreType.REGULAR((ROUNDS,)),
            ],
            compiler_params=pltpu.CompilerParams(
                collective_id=0, has_side_effects=True, vmem_limit_bytes=62 * 2**20),
            name="vocab_head",
        )(hidden.reshape(positions, depth), norm_w, draft_ids, embedding)
        return out[0], out[1]

    return jax.shard_map(local_part, mesh=mesh, in_specs=(P("dp", None, None), P(None), P("tp", None), P("dp", None)), out_specs=(P("dp", None), P("dp", None)), check_vma=False)
```

```python
import functools

import jax
import jax.numpy as jnp
from jax import lax
from jax.experimental import pallas as pl
from jax.experimental.pallas import tpu as pltpu
from jax.sharding import PartitionSpec as P

EPS = 1e-6
MESH = pl.DeviceIdType.MESH
SOLO_ROWS = 800
SOLO = 8
PAIR_ROWS = 832
PAIRS = 6
LANES = 128
SUB = 8
STATS = 4
QUARTERS = 4
ROUNDS = 5


def _stats_update(z, first_row, ids, stats):
    top, total, weighted, picked = stats
    rows, width = z.shape
    cube = z.reshape(rows // SUB, SUB, width)
    new_top = jnp.maximum(top, jnp.max(cube, axis=0))
    scale = jnp.exp(top - new_top)
    probs = jnp.exp(cube - new_top[None])
    total = total * scale + jnp.sum(probs, axis=0)
    weighted = weighted * scale + jnp.sum(probs * cube, axis=0)
    distance = ids - first_row - lax.broadcasted_iota(jnp.int32, (SUB, width), 0)
    for tile in range(rows // SUB):
        picked = jnp.where(distance == tile * SUB, cube[tile], picked)
    return new_top, total, weighted, picked


def _kernel(tp, hidden_hbm, gain_hbm, ids_hbm, emb_hbm, out_ref, hid, gain_vm, ids_vm, wts, outbox, inbox, ring, logits, mine, board,
            hid_sem, gain_sem, ids_sem, ids_sems, ring_sem, hop_send, hop_recv, swap_recv, send_sem, recv_sem, round_sem):
    me = lax.axis_index("tp")
    group = lax.axis_index("dp")
    parity = lax.rem(group, 2)
    other = group + 1 - 2 * parity
    core = lax.rem(me, 2)
    chip = me // 2
    chips = tp // 2
    shard_rows, depth = emb_hbm.shape
    columns = depth // 2
    pair_base = shard_rows - 2 * PAIRS * PAIR_ROWS
    lead_rows = pair_base - (SOLO - 1) * SOLO_ROWS
    _, seqs, drafts = out_ref.shape
    positions = seqs * drafts
    quarter = positions // QUARTERS
    tiles = quarter // SUB

    hid_copy = pltpu.make_async_copy(hidden_hbm, hid, hid_sem)
    gain_copy = pltpu.make_async_copy(gain_hbm, gain_vm, gain_sem)
    ids_copy = pltpu.make_async_copy(ids_hbm, ids_vm.at[0], ids_sem)
    hid_copy.start(priority=0)
    gain_copy.start(priority=0)
    ids_copy.start(priority=0)

    def solo_row(idx):
        return lead_rows + (idx - 1) * SOLO_ROWS

    def pair_row(idx):
        return pair_base + (parity * PAIRS + idx) * PAIR_ROWS

    def fetch(row, rows, slot):
        return pltpu.make_async_copy(emb_hbm.at[pl.ds(pl.multiple_of(row, 32), rows)], ring.at[slot, pl.ds(0, rows)], ring_sem.at[slot])

    def fetch_solo(idx):
        return fetch(solo_row(idx), SOLO_ROWS, idx)

    def fetch_pair(idx):
        return fetch(pair_row(idx), PAIR_ROWS, idx)

    fetch_lead = fetch(0, lead_rows, 0)
    fetch_lead.start(priority=1)
    for idx in range(1, SOLO):
        fetch_solo(idx).start(priority=1)

    all_steps = sorted(range(tp), key=lambda step: -min(step, tp - step))
    upper, lower = (2 * lax.rem(chip + shift, chips) + core for shift in (1, chips - 1))
    neighbours = (
        {"dp": other, "tp": me},
        {"dp": group, "tp": me + 1 - 2 * core},
        {"dp": group, "tp": upper},
        {"dp": group, "tp": lower},
    )

    def greet(semaphore):
        for device in neighbours:
            pl.semaphore_signal(semaphore, inc=1, device_id=device, device_id_type=MESH)

    def meet(turn):
        pl.semaphore_wait(round_sem.at[turn], len(neighbours))
        if turn + 1 < ROUNDS:
            greet(round_sem.at[turn + 1])

    barrier = pltpu.get_barrier_semaphore()
    greet(barrier)

    gain_copy.wait()
    hid_copy.wait()
    gain = 1.0 + gain_vm[...].astype(jnp.float32)[None]

    def normalize(x):
        x = x.astype(jnp.float32)
        mean_sq = jnp.sum(x * x, axis=-1, keepdims=True) / depth
        return (x * lax.rsqrt(mean_sq + EPS) * gain).astype(jnp.bfloat16)

    def quarter_of(turn):
        return lax.rem(chip + turn, QUARTERS)

    def prepare(turn):
        start = pl.multiple_of(quarter_of(turn) * quarter, quarter)
        normed = normalize(hid[pl.ds(start, quarter)])
        wts[pl.ds(start, quarter)] = normed
        if turn % 2 == 0:
            outbox[turn // 2] = normed.astype(jnp.float32)

    prepare(0)

    def spot(turn, tile, side):
        return inbox.at[quarter_of(turn), pl.ds(tile * SUB, SUB), pl.ds(pl.multiple_of(side * columns, columns), columns)]

    def hop(src, turn, tile, side, arrival, device):
        return pltpu.make_async_remote_copy(
            src_ref=src, dst_ref=spot(turn, tile, side), send_sem=hop_send, recv_sem=arrival,
            device_id=device, device_id_type=MESH)

    def across(turn, tile):
        src = outbox.at[turn // 2, pl.ds(tile * SUB, SUB), pl.ds(pl.multiple_of(core * columns, columns), columns)]
        return hop(src, turn, tile, core, hop_recv.at[turn * tiles + tile], {"dp": other, "tp": me})

    def along(tile, up):
        return hop(spot(0, tile, core), 0, tile, core, hop_recv.at[(3 if up else 1) * tiles + tile], {"dp": group, "tp": upper if up else lower})

    def sideways(turn, tile):
        return hop(spot(turn, tile, core), turn, tile, core, swap_recv, {"dp": group, "tp": me + 1 - 2 * core})

    def landed(turn, tile):
        hop(spot(turn, tile, core), turn, tile, core, hop_recv.at[turn * tiles + tile], {"dp": other, "tp": me}).wait_recv()

    ids_copy.wait()
    pl.semaphore_wait(barrier, len(neighbours))
    greet(round_sem.at[0])
    for tile in range(tiles):
        across(0, tile).start()
    prepare(2)
    for tile in range(tiles):
        across(2, tile).start()
    ids_hop = pltpu.make_async_remote_copy(
        src_ref=ids_vm.at[0], dst_ref=ids_vm.at[1], send_sem=ids_sems.at[0], recv_sem=ids_sems.at[1],
        device_id={"dp": other, "tp": me}, device_id_type=MESH)
    ids_hop.start()

    prepare(1)
    prepare(3)

    def pass_on(tile):
        landed(0, tile)
        along(tile, True).start()
        along(tile, False).start()

    def swap(turn, tile):
        if turn:
            landed(turn, tile)
        sideways(turn, tile).start()

    agenda = {
        3: [(pass_on, 0), (meet, 0)],
        4: [(pass_on, 1), (pass_on, 2)],
        5: [(pass_on, 3), (swap, 0, 0), (swap, 0, 1), (swap, 0, 2), (meet, 1)],
        6: [(swap, 0, 3), (swap, 2, 0), (swap, 2, 1), (swap, 1, 0), (swap, 3, 0)],
        7: [(swap, 1, 1), (swap, 3, 1), (swap, 1, 2), (swap, 3, 2), (swap, 2, 2), (swap, 1, 3), (swap, 3, 3), (swap, 2, 3), (meet, 2)],
    }

    def row_ids(which):
        table = ids_vm[which] - me * shard_rows
        return jnp.concatenate([table[seq:seq + 1] for seq in range(seqs)], axis=1)

    own_ids = row_ids(0)
    low = jnp.full((SUB, positions), jnp.finfo(jnp.float32).min, jnp.float32)
    zero = jnp.zeros((SUB, positions), jnp.float32)

    def multiply(slot, rows, width):
        stationary = wts[:width]
        half = rows // 2
        for part in range(2):
            span = slice(part * half, (part + 1) * half)
            logits[span, :width] = lax.dot_general(ring[slot, span], stationary, (((1,), (1,)), ((), ())), preferred_element_type=jnp.float32)

    def reduce(row, rows, width, ids, stats):
        return _stats_update(logits[:rows, :width], row, ids, stats)

    fetch_lead.wait()
    multiply(0, lead_rows, positions)
    fetch_pair(0).start(priority=1)

    fetch_solo(1).wait()
    stats = reduce(0, lead_rows, positions, own_ids, (low, zero, zero, zero))
    multiply(1, SOLO_ROWS, positions)
    fetch_pair(1).start(priority=1)

    def solo(idx, stats):
        for when, deeds in agenda.items():
            @pl.when(idx == when)
            def _(deeds=deeds):
                for deed, *what in deeds:
                    deed(*what)
        fetch_solo(idx).wait()
        stats = reduce(solo_row(idx - 1), SOLO_ROWS, positions, own_ids, stats)
        multiply(idx, SOLO_ROWS, positions)

        @pl.when(idx < PAIRS)
        def _():
            fetch_pair(idx).start(priority=1)

        return stats

    stats = lax.fori_loop(2, SOLO, solo, stats)

    half_box = inbox.at[pl.ds(0, QUARTERS // 2)]
    pltpu.make_async_copy(half_box, half_box, swap_recv).wait()
    ids_hop.wait_recv()
    wts[positions:] = inbox[...].reshape(positions, depth).astype(jnp.bfloat16)
    both_ids = jnp.concatenate([own_ids, row_ids(1)], axis=1)

    fetch_pair(0).wait()
    stats = reduce(solo_row(SOLO - 1), SOLO_ROWS, positions, own_ids, stats)
    multiply(0, PAIR_ROWS, 2 * positions)
    stats = tuple(jnp.concatenate([mine_part, start], axis=1) for mine_part, start in zip(stats, (low, zero, zero, zero)))

    def paired(idx, stats):
        for turn in range(3, ROUNDS):
            @pl.when(idx == 2 * turn - 4)
            def _(turn=turn):
                meet(turn)
        fetch_pair(idx).wait()
        stats = reduce(pair_row(idx - 1), PAIR_ROWS, 2 * positions, both_ids, stats)
        multiply(idx, PAIR_ROWS, 2 * positions)
        return stats

    stats = lax.fori_loop(1, PAIRS, paired, stats)
    top, total, weighted, picked = reduce(pair_row(PAIRS - 1), PAIR_ROWS, 2 * positions, both_ids, stats)

    best = jnp.max(top, axis=0, keepdims=True)
    scale = jnp.exp(top - best)
    summary = (
        best,
        jnp.sum(total * scale, axis=0, keepdims=True),
        jnp.sum(weighted * scale, axis=0, keepdims=True),
        jnp.sum(picked, axis=0, keepdims=True),
    )
    for side in range(2):
        for row, value in enumerate(summary):
            mine[side, row:row + 1] = value[:, side * positions:(side + 1) * positions]

    def report(side, step):
        return pltpu.make_async_remote_copy(
            src_ref=mine.at[side], dst_ref=board.at[side * tp + me], send_sem=send_sem, recv_sem=recv_sem,
            device_id={"dp": other if side else group, "tp": lax.rem(me + step, tp)}, device_id_type=MESH)

    for step in all_steps:
        report(1, step).start()
        if step:
            report(0, step).start()
    board[me] = mine[0]

    ids_hop.wait_send()
    pltpu.make_async_copy(inbox, inbox, hop_send).wait()
    others = board.at[pl.ds(0, 2 * tp - 1)]
    pltpu.make_async_copy(others, others, recv_sem).wait()
    pltpu.make_async_copy(others, others, send_sem).wait()

    every = board[...]
    tops = every[:, 0]
    row_max = jnp.max(tops, axis=0, keepdims=True)
    scale = jnp.exp(tops - row_max)
    exp_total = jnp.sum(every[:, 1] * scale, axis=0, keepdims=True)
    weighted = jnp.sum(every[:, 2] * scale, axis=0, keepdims=True)
    picked = jnp.sum(every[:, 3], axis=0, keepdims=True)
    log_norm = row_max + jnp.log(exp_total)
    log_prob = picked - log_norm
    entropy = log_norm - weighted / exp_total
    for seq in range(seqs):
        lanes = slice(seq * drafts, (seq + 1) * drafts)
        out_ref[0, seq:seq + 1] = log_prob[:, lanes]
        out_ref[1, seq:seq + 1] = entropy[:, lanes]


def solution(mesh):
    tp = mesh.shape["tp"]

    def local_part(hidden, norm_w, embedding, draft_ids):
        seqs, drafts, depth = hidden.shape
        positions = seqs * drafts
        tiles = positions // QUARTERS // SUB
        hbm = pl.BlockSpec(memory_space=pl.ANY)
        out = pl.pallas_call(
            functools.partial(_kernel, tp),
            out_shape=pltpu.VMEM((2, seqs, drafts), jnp.float32),
            in_specs=[hbm] * 4,
            out_specs=pl.BlockSpec(memory_space=pltpu.VMEM),
            scratch_shapes=[
                pltpu.VMEM((positions, depth), jnp.bfloat16),
                pltpu.VMEM((depth,), jnp.bfloat16),
                pltpu.VMEM((2, seqs, drafts), jnp.int32),
                pltpu.VMEM((2 * positions, depth), jnp.bfloat16),
                pltpu.VMEM((2, positions // QUARTERS, depth), jnp.float32),
                pltpu.VMEM((QUARTERS, positions // QUARTERS, depth), jnp.float32),
                pltpu.VMEM((SOLO, PAIR_ROWS, depth), jnp.bfloat16),
                pltpu.VMEM((PAIR_ROWS, 2 * positions), jnp.float32),
                pltpu.VMEM((2, STATS, positions), jnp.float32),
                pltpu.VMEM((2 * tp, STATS, positions), jnp.float32),
                pltpu.SemaphoreType.DMA,
                pltpu.SemaphoreType.DMA,
                pltpu.SemaphoreType.DMA,
                pltpu.SemaphoreType.DMA((2,)),
                pltpu.SemaphoreType.DMA((SOLO,)),
                pltpu.SemaphoreType.DMA,
                pltpu.SemaphoreType.DMA((QUARTERS * tiles,)),
                pltpu.SemaphoreType.DMA,
                pltpu.SemaphoreType.DMA,
                pltpu.SemaphoreType.DMA,
                pltpu.SemaphoreType.REGULAR((ROUNDS,)),
            ],
            compiler_params=pltpu.CompilerParams(
                collective_id=0, has_side_effects=True, vmem_limit_bytes=62 * 2**20),
            name="vocab_head",
        )(hidden.reshape(positions, depth), norm_w, draft_ids, embedding)
        return out[0], out[1]

    return jax.shard_map(local_part, mesh=mesh, in_specs=(P("dp", None, None), P(None), P("tp", None), P("dp", None)), out_specs=(P("dp", None), P("dp", None)), check_vma=False)
```
